32 devices in a mesh: shift: 16 (over z, x, core), row: 2 (over y).
Axes of the slice: x: 2, y: 2, z: 4, core: 2. Of those that a mesh axis runs over, the one named last changes fastest.
Arguments:
- solutions: bfloat16 [32, 2, 2048, 128], P('shift', None, 'row'), may hold values from -96 to 96
Outputs:
- moments: bfloat16 [2, 8, 2048, 128], P(None, None, ('row', 'shift'))
- gram_real: float32 [1024, 1024], replicated
- gram_imag: float32 [1024, 1024], replicated
The draws below stay inside these ranges and needn't reach their ends.
All inputs are finite; a program needn't handle non-finite values.
Results may differ from the reference program's by a relative error of at most 0.0061.
Values may be sent and summed in bfloat16 or wider, within the bound.
A program may use at most 64 MiB of HBM per device.

```python
import math
import jax
import jax.numpy as jnp
from jax import lax

SOURCES = 128
PANELS = 8
SHIFTS = 32
ROWS = 2048


def spiked(entries, key, source, target, blocks, factor):
    def block_of(axis_at):
        return (jnp.arange(entries.shape[axis_at]) // (entries.shape[axis_at] // blocks)).reshape((-1,) + (1,) * (entries.ndim - 1 - axis_at))

    near = jax.random.permutation(key, blocks)[block_of(target)]
    far = (block_of(target) + blocks // 2) % blocks
    return jnp.where((block_of(source) == near) | (block_of(source) == far), factor * entries, entries)


def shard_levels(own_key, shape, cuts, smallest, high):
    def one(position, parts):
        heights = jax.random.uniform(jax.random.fold_in(jax.random.fold_in(own_key, 6), position), (parts,), jnp.float32, smallest / len(cuts), high / len(cuts))
        return jnp.repeat(jnp.exp(heights), shape[position] // parts).reshape((-1,) + (1,) * (len(shape) - position - 1))

    loudness = one(*cuts[0])
    for cut in cuts[1:]:
        loudness = loudness * one(*cut)
    return loudness


def gaussian_with(rng, dims, scale, most, pieces, heavy, held_as=jnp.bfloat16):
    drawn = scale * jax.random.normal(rng, dims, jnp.float32)
    if pieces:
        drawn = drawn * shard_levels(rng, dims, pieces, -0.22, 0.18)
    return jnp.clip(spiked(drawn, jax.random.fold_in(rng, 3), *heavy), -most, most).astype(held_as)


def setup_inputs(seed: int = 0) -> dict:
    key_of = jax.random.split(jax.random.key(seed), 2)
    solutions = gaussian_with(key_of[0], (SHIFTS, 2, ROWS, SOURCES), 16.0, 96.0, ((0, 16), (2, 2)), (0, 2, 16, 2.0))
    return {"solutions": solutions}


def coefficient_block(first_shift, shift_count, all_shifts, panels):
    indices = (first_shift + jnp.arange(shift_count, dtype=jnp.int32)).astype(jnp.float32)
    orders = jnp.arange(1, panels + 1, dtype=jnp.int32).astype(jnp.float32)
    angles = orders[:, None] * (2.0 * math.pi * (indices + 0.5) / all_shifts)[None, :]
    cos_part = jnp.cos(angles) / all_shifts
    sin_part = jnp.sin(angles) / all_shifts
    real_row = jnp.stack([cos_part, -sin_part], axis=-1)
    imag_row = jnp.stack([sin_part, cos_part], axis=-1)
    return jnp.stack([real_row, imag_row], axis=0).reshape(2 * panels, 2 * shift_count).astype(jnp.bfloat16)

def pair_product(left, right):
    width = left.shape[0] * left.shape[2]
    return jnp.einsum('krl,qrm->klqm', left.astype(jnp.float32), right.astype(jnp.float32), precision=lax.Precision.HIGHEST).reshape(width, width)

def reference(solutions):
    weights = coefficient_block(0, SHIFTS, SHIFTS, PANELS)
    flat = solutions.reshape(2 * SHIFTS, ROWS * SOURCES)
    moment_sum = jnp.dot(weights, flat, preferred_element_type=jnp.float32).reshape(2, PANELS, ROWS, SOURCES)
    moments = moment_sum.astype(jnp.bfloat16)
    real_part = moments[0]
    imag_part = moments[1]
    gram_real = pair_product(real_part, real_part) + pair_product(imag_part, imag_part)
    gram_imag = pair_product(real_part, imag_part) - pair_product(imag_part, real_part)
    factor = 1.0 / math.sqrt(ROWS)
    return (moments, gram_real * factor, gram_imag * factor)
```

```python
import functools
import math

import jax
import jax.numpy as jnp
import numpy as np
from jax import lax
from jax.experimental import pallas as pl
from jax.experimental.pallas import tpu as pltpu
from jax.sharding import PartitionSpec as P

PANELS = 8
PAIRS = PANELS * (PANELS // 2) + PANELS // 2
OUTS = 2 * PANELS
RELAY_LAG = 4
DIAGONAL_LAG = 7
MESH = pl.DeviceIdType.MESH


def coefficients(all_shifts, owners):
    indices = np.arange(all_shifts, dtype=np.float32)
    orders = np.arange(1, PANELS + 1, dtype=np.float32)
    step = (np.float32(2.0 * math.pi) * (indices + np.float32(0.5)) / np.float32(all_shifts)).astype(np.float32)
    angles = (orders[:, None] * step[None, :]).astype(np.float32).astype(np.float64)
    cos_part = np.cos(angles).astype(np.float32) / np.float32(all_shifts)
    sin_part = np.sin(angles).astype(np.float32) / np.float32(all_shifts)
    real_row = np.stack([cos_part, -sin_part], axis=-1)
    imag_row = np.stack([sin_part, cos_part], axis=-1)
    both = np.stack([real_row, imag_row], axis=0).reshape(OUTS, owners, -1)
    return both.transpose(1, 0, 2).reshape(-1).astype(jnp.bfloat16).astype(np.float32)


def units_per_core(R):
    t = -(-2 * PAIRS // (4 * R))
    return t + 1 - t % 2


def exchange(
    N, R, rows, part, T, factor,
    w_hbm, x_hbm, m_ref, ag,
    w_ref, x_ref, xs, sbuf, own, dout, din, fo, up, fm,
    in_sems, a2a_s, a2a_r, sg_s, sg_r, dd_s, dd_r, up_s, fo_r, out_s, in_r, ag_s, ag_r,
):
    Z = N // 4
    CH = rows // part
    s = lax.axis_index("shift")
    r = lax.axis_index("row")
    core = lax.rem(s, 2)
    z = s // 4
    x = lax.rem(s // 2, 2)
    inputs = x_ref.shape[0]
    width = x_ref.shape[2]
    cut = width // 2
    slots = 2 * R

    def member(x_, r_, c_):
        return (r_ * 2 + x_) * 2 + c_

    def place(z_, x_, c_):
        return (z_ * 2 + x_) * 2 + c_

    p = member(x, r, core)
    here = r * 2 + x
    partner = place(z, x, 1 - core)
    across = place(z, 1 - x, core)

    def row_at(i):
        return lax.rem(r + i + R, R)

    def remote(src, dst, ss, rr, to_s, to_r):
        return pltpu.make_async_remote_copy(
            src_ref=src, dst_ref=dst, send_sem=ss, recv_sem=rr,
            device_id={"shift": to_s, "row": to_r}, device_id_type=MESH,
        )

    load_x = pltpu.make_async_copy(x_hbm, x_ref, in_sems.at[0])
    load_w = pltpu.make_async_copy(w_hbm, w_ref, in_sems.at[1])
    load_x.start()
    load_w.start()
    barrier = pltpu.get_barrier_semaphore()
    for i in range(1, N):
        pl.semaphore_signal(barrier, inc=1, device_id={"shift": lax.rem(s + i, N), "row": r}, device_id_type=MESH)
    for i in range(1, R):
        for to in (s, across):
            pl.semaphore_signal(barrier, inc=1, device_id={"shift": to, "row": row_at(i)}, device_id_type=MESH)
    load_x.wait()
    load_w.wait()
    pl.semaphore_wait(barrier, N - 1 + 2 * (R - 1))


    def rows_of(owner, h):
        return pl.ds(pl.multiple_of(owner * rows + h * part, part), part)

    def a2a_send(h, to):
        return remote(x_ref.at[:, rows_of(to, h), :], xs.at[h, s], a2a_s.at[h, to], a2a_r.at[h, s], to, r)

    def a2a_arrive(h, source):
        remote(xs.at[h, source], xs.at[h, source], a2a_s.at[h, source], a2a_r.at[h, source], s, r).wait_recv()

    for e in range(Z // 2):
        def send_chunk(h, c, e=e):
            for to_z in (e, Z - 1 - e):
                for dx, dc in ((0, 0), (1, 0), (0, 1), (1, 1)):
                    to = place(to_z, lax.rem(x + dx, 2), lax.rem(core + dc, 2))
                    if dx or dc:
                        a2a_send(h, to).start()
                    else:
                        @pl.when(to_z != z)
                        def _():
                            a2a_send(h, to).start()
            return c

        lax.fori_loop(0, CH, send_chunk, 0)


    def weigh(acc, blocks, source):
        parts = [b.astype(jnp.float32) for b in blocks]
        out = []
        for o in range(OUTS):
            base = (source * OUTS + o) * inputs
            total = parts[0] * w_ref[base]
            for c in range(1, inputs):
                total += parts[c] * w_ref[base + c]
            out.append(total if acc is None else acc[o] + total)
        return tuple(out)

    def gather(h, to_x, to_r):
        k = lax.rem(to_r - r + R, R) * 2 + lax.rem(to_x + x, 2)
        return remote(
            sbuf.at[h, here], sbuf.at[h, here], sg_s.at[h, k], sg_r.at[h, here], place(z, to_x, core), to_r,
        )

    peers = [(i, j) for i in range(R) for j in range(2) if i or j]

    def moments_of(h, c):
        acc = weigh(None, [x_ref[q, rows_of(s, h), :] for q in range(inputs)], s)

        def take(j, acc):
            source = lax.rem(s - 1 - j + N, N)
            a2a_arrive(h, source)
            return weigh(acc, [xs[h, source, q] for q in range(inputs)], source)

        acc = lax.fori_loop(0, N - 1, take, acc)
        at = pl.ds(pl.multiple_of(h * part, part), part)
        for o in range(OUTS):
            value = acc[o].astype(jnp.bfloat16)
            sbuf[h, here, o] = value
            m_ref[o, at, :] = value
        for i, j in peers:
            gather(h, lax.rem(x + j, 2), row_at(i)).start()
        return c

    lax.fori_loop(0, CH, moments_of, 0)

    def gathered(h, c):
        for i, j in peers:
            slot = row_at(i) * 2 + lax.rem(x + j, 2)
            remote(sbuf.at[h, slot], sbuf.at[h, slot], sg_s.at[h, 0], sg_r.at[h, slot], s, r).wait_recv()
        return c

    lax.fori_loop(0, CH, gathered, 0)


    depth = slots * rows
    middle = T // 2
    toward = 1 - 2 * core
    dims = (((0,), (0,)), ((), ()))

    def pair(j):
        u = jnp.minimum(here * T + j, PAIRS - 1)
        k = lax.rem(u, PANELS)
        q = lax.rem(k + u // PANELS, PANELS)
        lr = sbuf[:, :, k].reshape(depth, width)
        li = sbuf[:, :, PANELS + k].reshape(depth, width)
        rr = sbuf[:, :, q].reshape(depth, width)
        ri = sbuf[:, :, PANELS + q].reshape(depth, width)
        out = lax.dot_general(
            lr, jnp.concatenate([rr, ri], axis=1), dims, preferred_element_type=jnp.float32
        ) + lax.dot_general(
            li, jnp.concatenate([ri, -rr], axis=1), dims, preferred_element_type=jnp.float32
        )
        out = out * factor
        return out[:cut], out[cut:]

    def pick(a, b):
        return jnp.where(core == 0, a, b)

    def swap(t):
        return remote(dout.at[t], din.at[t], dd_s.at[t], dd_r.at[t], partner, r)

    low, high = pair(middle)
    dout[0] = pick(high, low).astype(jnp.bfloat16)
    own[0] = pick(low, high)
    swap(0).start()

    def theirs(n, c):
        low, high = pair(middle + toward * (n + 1))
        dout[2 * n + 1] = pick(low, high).astype(jnp.bfloat16)
        dout[2 * n + 2] = pick(high, low).astype(jnp.bfloat16)
        swap(2 * n + 1).start()
        swap(2 * n + 2).start()
        return c

    lax.fori_loop(0, middle, theirs, 0)

    def mine(n, c):
        low, high = pair(middle - toward * (n + 1))
        own[2 * n + 1] = pick(high, low)
        own[2 * n + 2] = pick(low, high)
        return c

    lax.fori_loop(0, middle, mine, 0)


    lower = z < Z // 2
    inner = jnp.where(lower, z + 1, z - 1)
    outer = jnp.where(lower, z - 1, z + 1)
    from_end = jnp.where(lower, z, Z - 1 - z)
    is_middle = from_end == Z // 2 - 1
    has_outer = from_end > 0
    inner_s = place(inner, x, core)
    outer_s = place(jnp.where(has_outer, outer, inner), x, core)

    def to_mate(t):
        return remote(up.at[t], fm.at[t], up_s.at[t], in_r.at[t], inner_s, r)

    def to_inner(t):
        return remote(up.at[t], fo.at[t], up_s.at[t], fo_r.at[t], inner_s, r)

    def to_outer(t):
        return remote(ag.at[p, t], ag.at[p, t], out_s.at[t], in_r.at[t], outer_s, r)

    def climb(t, c):
        swap(t).wait_recv()
        own[t] = own[t] + din[t].astype(jnp.float32)

        @pl.when(has_outer)
        def _():
            remote(fo.at[t], fo.at[t], up_s.at[t], fo_r.at[t], s, r).wait_recv()
            own[t] = own[t] + fo[t].astype(jnp.float32)

        up[t] = own[t].astype(jnp.bfloat16)

        @pl.when(is_middle)
        def _():
            to_mate(t).start()

        @pl.when(jnp.logical_not(is_middle))
        def _():
            to_inner(t).start()

        return c

    lax.fori_loop(0, T, climb, 0)


    counts = [0]
    done = []

    def copy(t, slot, ss, to_s, to_r):
        return remote(ag.at[slot, t], ag.at[slot, t], ss, ag_r.at[t, slot], to_s, to_r)

    def forward(t, slot, to_s, to_r):
        c = copy(t, slot, ag_s.at[counts[0]], to_s, to_r)
        counts[0] += 1
        c.start()
        done.append(c)

    def arrive(t, slot):
        copy(t, slot, ag_s.at[0], s, r).wait_recv()

    def total(t):
        @pl.when(is_middle)
        def _():
            remote(fm.at[t], fm.at[t], up_s.at[t], in_r.at[t], s, r).wait_recv()
            ag[p, t] = (up[t].astype(jnp.float32) + fm[t].astype(jnp.float32)).astype(jnp.bfloat16)

        @pl.when(jnp.logical_not(is_middle))
        def _():
            remote(ag.at[p, t], ag.at[p, t], up_s.at[t], in_r.at[t], s, r).wait_recv()

        @pl.when(has_outer)
        def _():
            to_outer(t).start()

    def spread(t):
        forward(t, p, across, r)
        for i in range(1, R):
            forward(t, p, s, row_at(i))
        forward(t, p, partner, r)

    def relay(t):
        arrive(t, member(1 - x, r, core))
        for i in range(1, R):
            arrive(t, member(x, row_at(-i), core))
        first = core == 0
        for i in range(1, R):
            slot = jnp.where(first, member(1 - x, r, core), member(x, row_at(-i), core))
            forward(t, slot, jnp.where(first, s, across), jnp.where(first, row_at(i), r))
        forward(t, member(1 - x, r, core), partner, r)
        for i in range(1, R):
            forward(t, member(x, row_at(-i), core), partner, r)

    def diagonal(t):
        for i in range(1, R):
            slot = member(1 - x, row_at(-i), core)
            arrive(t, slot)
            forward(t, slot, partner, r)

    def rest(t):
        for i in range(R):
            for o in range(2):
                arrive(t, member(lax.rem(x + o, 2), row_at(i), 1 - core))

    for n in range(T + DIAGONAL_LAG):
        if n < T:
            total(n)
            spread(n)
        if 0 <= n - RELAY_LAG < T:
            relay(n - RELAY_LAG)
        if 0 <= n - DIAGONAL_LAG < T:
            diagonal(n - DIAGONAL_LAG)
    for t in range(T):
        rest(t)


    def drain(h, c):
        for i in range(1, N):
            a2a_send(h, lax.rem(s + i, N)).wait_send()
        for i, j in peers:
            gather(h, lax.rem(x + j, 2), row_at(i)).wait_send()
        return c

    lax.fori_loop(0, CH, drain, 0)

    def drain_units(t, c):
        swap(t).wait_send()
        to_inner(t).wait_send()

        @pl.when(has_outer)
        def _():
            to_outer(t).wait_send()

        return c

    lax.fori_loop(0, T, drain_units, 0)
    for c in done:
        c.wait_send()


def expand(T, m_in, ag_ref, m_out, re_out, im_out, re_buf, im_buf, sems, m_sem):
    width = re_buf.shape[1]
    half = PANELS // 2
    keep = pltpu.make_async_copy(m_in, m_out, m_sem)
    keep.start()

    def unit(n):
        chip = n // (2 * T)
        v = lax.rem(n, 2 * T)
        low = v < T
        value = ag_ref[2 * chip + jnp.where(low, 0, 1), jnp.where(low, T - 1 - v, v - T)]
        return value.astype(jnp.float32)

    def pair(u):
        return jnp.concatenate([unit(2 * u), unit(2 * u + 1)], axis=0)

    def writes(k, slot):
        at = pl.ds(pl.multiple_of(k * width, width), width)
        return (
            pltpu.make_async_copy(re_buf.at[k], re_out.at[at], sems.at[0, k]),
            pltpu.make_async_copy(im_buf.at[k], im_out.at[at], sems.at[1, k]),
        )

    def one(k, c):
        for d in range(PANELS):
            q = lax.rem(k + d, PANELS)
            at = pl.ds(pl.multiple_of(q * width, width), width)
            if d < half:
                v = pair(PANELS * d + k)
                re, im = v[:, :width], v[:, width:]
            elif d == half:
                v = pair(PANELS * half + jnp.minimum(k, q))
                re, im = v[:, :width], v[:, width:]
                re, im = jnp.where(k < half, re, re.T), jnp.where(k < half, im, -im.T)
            else:
                v = pair(PANELS * (PANELS - d) + q)
                re, im = v[:, :width].T, -v[:, width:].T
            re_buf[k, :, at] = re
            im_buf[k, :, at] = im
        for copy in writes(k, k):
            copy.start()
        return c

    lax.fori_loop(0, PANELS, one, 0)

    def finish(k, c):
        for copy in writes(k, k):
            copy.wait()
        return c

    lax.fori_loop(0, PANELS, finish, 0)
    keep.wait()


def local(N, R, solutions):
    shifts, parts, height, width = solutions.shape
    rows = height // N
    T = units_per_core(R)
    G = 4 * R
    cut = width // 2
    inputs = shifts * parts
    part = 16 if rows % 16 == 0 else rows
    chunks = rows // part
    factor = 1.0 / math.sqrt(height * R)
    w = jnp.asarray(coefficients(shifts * N, N))
    bf, dma = jnp.bfloat16, pltpu.SemaphoreType.DMA
    vmem = pl.BlockSpec(memory_space=pltpu.VMEM)
    hbm = pl.BlockSpec(memory_space=pltpu.HBM)
    unit = (T, cut, 2 * width)
    spreads = T * (1 + (R - 1) + 1 + (R - 1) + 1 + (R - 1) + (R - 1))
    moments, parts_of_gram = pl.pallas_call(
        functools.partial(exchange, N, R, rows, part, T, factor),
        out_shape=(
            jax.ShapeDtypeStruct((OUTS, rows, width), bf),
            jax.ShapeDtypeStruct((G,) + unit, bf),
        ),
        in_specs=[hbm, hbm],
        out_specs=(vmem, vmem),
        scratch_shapes=[
            pltpu.SMEM(w.shape, jnp.float32),
            pltpu.VMEM((inputs, height, width), bf),
            pltpu.VMEM((chunks, N, inputs, part, width), bf),
            pltpu.VMEM((chunks, 2 * R, OUTS, part, width), bf),
            pltpu.VMEM(unit, jnp.float32),
            pltpu.VMEM(unit, bf), pltpu.VMEM(unit, bf), pltpu.VMEM(unit, bf),
            pltpu.VMEM(unit, bf), pltpu.VMEM(unit, bf),
            dma((2,)),
            dma((chunks, N)), dma((chunks, N)), dma((chunks, 2 * R)), dma((chunks, 2 * R)),
            dma((T,)), dma((T,)), dma((T,)), dma((T,)), dma((T,)), dma((T,)),
            dma((spreads,)), dma((T, G)),
        ],
        compiler_params=pltpu.CompilerParams(
            collective_id=0, has_side_effects=True, vmem_limit_bytes=32 * 2**20
        ),
        cost_estimate=pl.CostEstimate(flops=10**9, bytes_accessed=2**23, transcendentals=0),
    )(w, solutions.reshape(inputs, height, width))
    size = PANELS * width
    anywhere = pl.BlockSpec(memory_space=pl.ANY)
    moments, gram_real, gram_imag = pl.pallas_call(
        functools.partial(expand, T),
        out_shape=(
            jax.ShapeDtypeStruct((OUTS, rows, width), bf),
            jax.ShapeDtypeStruct((size, size), jnp.float32),
            jax.ShapeDtypeStruct((size, size), jnp.float32),
        ),
        in_specs=[vmem, vmem],
        out_specs=(anywhere, anywhere, anywhere),
        scratch_shapes=[
            pltpu.VMEM((PANELS, width, size), jnp.float32),
            pltpu.VMEM((PANELS, width, size), jnp.float32),
            dma((2, PANELS)),
            dma,
        ],
        compiler_params=pltpu.CompilerParams(vmem_limit_bytes=32 * 2**20),
        cost_estimate=pl.CostEstimate(flops=10**7, bytes_accessed=2**24, transcendentals=0),
    )(moments, parts_of_gram)
    return moments.reshape(2, PANELS, rows, width), gram_real, gram_imag


def solution(mesh):
    return jax.shard_map(
        functools.partial(local, mesh.shape["shift"], mesh.shape["row"]),
        mesh=mesh,
        in_specs=(P("shift", None, "row", None),),
        out_specs=(P(None, None, ("row", "shift"), None), P(), P()),
        check_vma=False,
    )
```

```python
import functools
import math

import jax
import jax.numpy as jnp
import numpy as np
from jax import lax
from jax.experimental import pallas as pl
from jax.experimental.pallas import tpu as pltpu
from jax.sharding import PartitionSpec as P

PANELS = 8
PAIRS = PANELS * (PANELS // 2) + PANELS // 2
OUTS = 2 * PANELS
RELAY_LAG = 4
DIAGONAL_LAG = 7
MESH = pl.DeviceIdType.MESH


def coefficients(all_shifts, owners):
    indices = np.arange(all_shifts, dtype=np.float32)
    orders = np.arange(1, PANELS + 1, dtype=np.float32)
    step = (np.float32(2.0 * math.pi) * (indices + np.float32(0.5)) / np.float32(all_shifts)).astype(np.float32)
    angles = (orders[:, None] * step[None, :]).astype(np.float32).astype(np.float64)
    cos_part = np.cos(angles).astype(np.float32) / np.float32(all_shifts)
    sin_part = np.sin(angles).astype(np.float32) / np.float32(all_shifts)
    real_row = np.stack([cos_part, -sin_part], axis=-1)
    imag_row = np.stack([sin_part, cos_part], axis=-1)
    both = np.stack([real_row, imag_row], axis=0).reshape(OUTS, owners, -1)
    return both.transpose(1, 0, 2).reshape(-1).astype(jnp.bfloat16).astype(np.float32)


def units_per_core(R):
    t = -(-2 * PAIRS // (4 * R))
    return t + 1 - t % 2


def exchange(
    N, R, rows, part, T, factor,
    w_hbm, x_hbm, m_ref, ag,
    w_ref, x_ref, xs, sbuf, own, dout, din, fo, up, fm,
    in_sems, a2a_s, a2a_r, sg_s, sg_r, dd_s, dd_r, up_s, fo_r, out_s, in_r, ag_s, ag_r,
):
    Z = N // 4
    CH = rows // part
    s = lax.axis_index("shift")
    r = lax.axis_index("row")
    core = lax.rem(s, 2)
    z = s // 4
    x = lax.rem(s // 2, 2)
    inputs = x_ref.shape[0]
    width = x_ref.shape[2]
    cut = width // 2
    slots = 2 * R

    def member(x_, r_, c_):
        return (r_ * 2 + x_) * 2 + c_

    def place(z_, x_, c_):
        return (z_ * 2 + x_) * 2 + c_

    p = member(x, r, core)
    here = r * 2 + x
    partner = place(z, x, 1 - core)
    across = place(z, 1 - x, core)

    def row_at(i):
        return lax.rem(r + i + R, R)

    def remote(src, dst, ss, rr, to_s, to_r):
        return pltpu.make_async_remote_copy(
            src_ref=src, dst_ref=dst, send_sem=ss, recv_sem=rr,
            device_id={"shift": to_s, "row": to_r}, device_id_type=MESH,
        )

    load_x = pltpu.make_async_copy(x_hbm, x_ref, in_sems.at[0])
    load_w = pltpu.make_async_copy(w_hbm, w_ref, in_sems.at[1])
    load_x.start()
    load_w.start()
    barrier = pltpu.get_barrier_semaphore()
    for i in range(1, N):
        pl.semaphore_signal(barrier, inc=1, device_id={"shift": lax.rem(s + i, N), "row": r}, device_id_type=MESH)
    for i in range(1, R):
        for to in (s, across):
            pl.semaphore_signal(barrier, inc=1, device_id={"shift": to, "row": row_at(i)}, device_id_type=MESH)
    load_x.wait()
    load_w.wait()
    pl.semaphore_wait(barrier, N - 1 + 2 * (R - 1))


    def rows_of(owner, h):
        return pl.ds(pl.multiple_of(owner * rows + h * part, part), part)

    def a2a_send(h, to):
        return remote(x_ref.at[:, rows_of(to, h), :], xs.at[h, s], a2a_s.at[h, to], a2a_r.at[h, s], to, r)

    def a2a_arrive(h, source):
        remote(xs.at[h, source], xs.at[h, source], a2a_s.at[h, source], a2a_r.at[h, source], s, r).wait_recv()

    for e in range(Z // 2):
        def send_chunk(h, c, e=e):
            for to_z in (e, Z - 1 - e):
                for dx, dc in ((0, 0), (1, 0), (0, 1), (1, 1)):
                    to = place(to_z, lax.rem(x + dx, 2), lax.rem(core + dc, 2))
                    if dx or dc:
                        a2a_send(h, to).start()
                    else:
                        @pl.when(to_z != z)
                        def _():
                            a2a_send(h, to).start()
            return c

        lax.fori_loop(0, CH, send_chunk, 0)


    def weigh(acc, blocks, source):
        parts = [b.astype(jnp.float32) for b in blocks]
        out = []
        for o in range(OUTS):
            base = (source * OUTS + o) * inputs
            total = parts[0] * w_ref[base]
            for c in range(1, inputs):
                total += parts[c] * w_ref[base + c]
            out.append(total if acc is None else acc[o] + total)
        return tuple(out)

    def gather(h, to_x, to_r):
        k = lax.rem(to_r - r + R, R) * 2 + lax.rem(to_x + x, 2)
        return remote(
            sbuf.at[h, here], sbuf.at[h, here], sg_s.at[h, k], sg_r.at[h, here], place(z, to_x, core), to_r,
        )

    peers = [(i, j) for i in range(R) for j in range(2) if i or j]

    def moments_of(h, c):
        acc = weigh(None, [x_ref[q, rows_of(s, h), :] for q in range(inputs)], s)

        def take(j, acc):
            source = lax.rem(s - 1 - j + N, N)
            a2a_arrive(h, source)
            return weigh(acc, [xs[h, source, q] for q in range(inputs)], source)

        acc = lax.fori_loop(0, N - 1, take, acc)
        at = pl.ds(pl.multiple_of(h * part, part), part)
        for o in range(OUTS):
            value = acc[o].astype(jnp.bfloat16)
            sbuf[h, here, o] = value
            m_ref[o, at, :] = value
        for i, j in peers:
            gather(h, lax.rem(x + j, 2), row_at(i)).start()
        return c

    lax.fori_loop(0, CH, moments_of, 0)

    def gathered(h, c):
        for i, j in peers:
            slot = row_at(i) * 2 + lax.rem(x + j, 2)
            remote(sbuf.at[h, slot], sbuf.at[h, slot], sg_s.at[h, 0], sg_r.at[h, slot], s, r).wait_recv()
        return c

    lax.fori_loop(0, CH, gathered, 0)


    depth = slots * rows
    middle = T // 2
    toward = 1 - 2 * core
    dims = (((0,), (0,)), ((), ()))

    def pair(j):
        u = jnp.minimum(here * T + j, PAIRS - 1)
        k = lax.rem(u, PANELS)
        q = lax.rem(k + u // PANELS, PANELS)
        lr = sbuf[:, :, k].reshape(depth, width)
        li = sbuf[:, :, PANELS + k].reshape(depth, width)
        rr = sbuf[:, :, q].reshape(depth, width)
        ri = sbuf[:, :, PANELS + q].reshape(depth, width)
        out = lax.dot_general(
            lr, jnp.concatenate([rr, ri], axis=1), dims, preferred_element_type=jnp.float32
        ) + lax.dot_general(
            li, jnp.concatenate([ri, -rr], axis=1), dims, preferred_element_type=jnp.float32
        )
        out = out * factor
        return out[:cut], out[cut:]

    def pick(a, b):
        return jnp.where(core == 0, a, b)

    def swap(t):
        return remote(dout.at[t], din.at[t], dd_s.at[t], dd_r.at[t], partner, r)

    low, high = pair(middle)
    dout[0] = pick(high, low).astype(jnp.bfloat16)
    own[0] = pick(low, high)
    swap(0).start()

    def theirs(n, c):
        low, high = pair(middle + toward * (n + 1))
        dout[2 * n + 1] = pick(low, high).astype(jnp.bfloat16)
        dout[2 * n + 2] = pick(high, low).astype(jnp.bfloat16)
        swap(2 * n + 1).start()
        swap(2 * n + 2).start()
        return c

    lax.fori_loop(0, middle, theirs, 0)

    def mine(n, c):
        low, high = pair(middle - toward * (n + 1))
        own[2 * n + 1] = pick(high, low)
        own[2 * n + 2] = pick(low, high)
        return c

    lax.fori_loop(0, middle, mine, 0)


    lower = z < Z // 2
    inner = jnp.where(lower, z + 1, z - 1)
    outer = jnp.where(lower, z - 1, z + 1)
    from_end = jnp.where(lower, z, Z - 1 - z)
    is_middle = from_end == Z // 2 - 1
    has_outer = from_end > 0
    inner_s = place(inner, x, core)
    outer_s = place(jnp.where(has_outer, outer, inner), x, core)

    def to_mate(t):
        return remote(up.at[t], fm.at[t], up_s.at[t], in_r.at[t], inner_s, r)

    def to_inner(t):
        return remote(up.at[t], fo.at[t], up_s.at[t], fo_r.at[t], inner_s, r)

    def to_outer(t):
        return remote(ag.at[p, t], ag.at[p, t], out_s.at[t], in_r.at[t], outer_s, r)

    def climb(t, c):
        swap(t).wait_recv()
        own[t] = own[t] + din[t].astype(jnp.float32)

        @pl.when(has_outer)
        def _():
            remote(fo.at[t], fo.at[t], up_s.at[t], fo_r.at[t], s, r).wait_recv()
            own[t] = own[t] + fo[t].astype(jnp.float32)

        up[t] = own[t].astype(jnp.bfloat16)

        @pl.when(is_middle)
        def _():
            to_mate(t).start()

        @pl.when(jnp.logical_not(is_middle))
        def _():
            to_inner(t).start()

        return c

    lax.fori_loop(0, T, climb, 0)


    counts = [0]
    done = []

    def copy(t, slot, ss, to_s, to_r):
        return remote(ag.at[slot, t], ag.at[slot, t], ss, ag_r.at[t, slot], to_s, to_r)

    def forward(t, slot, to_s, to_r):
        c = copy(t, slot, ag_s.at[counts[0]], to_s, to_r)
        counts[0] += 1
        c.start()
        done.append(c)

    def arrive(t, slot):
        copy(t, slot, ag_s.at[0], s, r).wait_recv()

    def total(t):
        @pl.when(is_middle)
        def _():
            remote(fm.at[t], fm.at[t], up_s.at[t], in_r.at[t], s, r).wait_recv()
            ag[p, t] = (up[t].astype(jnp.float32) + fm[t].astype(jnp.float32)).astype(jnp.bfloat16)

        @pl.when(jnp.logical_not(is_middle))
        def _():
            remote(ag.at[p, t], ag.at[p, t], up_s.at[t], in_r.at[t], s, r).wait_recv()

        @pl.when(has_outer)
        def _():
            to_outer(t).start()

    def spread(t):
        forward(t, p, across, r)
        for i in range(1, R):
            forward(t, p, s, row_at(i))
        forward(t, p, partner, r)

    def relay(t):
        arrive(t, member(1 - x, r, core))
        for i in range(1, R):
            arrive(t, member(x, row_at(-i), core))
        first = core == 0
        for i in range(1, R):
            slot = jnp.where(first, member(1 - x, r, core), member(x, row_at(-i), core))
            forward(t, slot, jnp.where(first, s, across), jnp.where(first, row_at(i), r))
        forward(t, member(1 - x, r, core), partner, r)
        for i in range(1, R):
            forward(t, member(x, row_at(-i), core), partner, r)

    def diagonal(t):
        for i in range(1, R):
            slot = member(1 - x, row_at(-i), core)
            arrive(t, slot)
            forward(t, slot, partner, r)

    def rest(t):
        for i in range(R):
            for o in range(2):
                arrive(t, member(lax.rem(x + o, 2), row_at(i), 1 - core))

    for n in range(T + DIAGONAL_LAG):
        if n < T:
            total(n)
            spread(n)
        if 0 <= n - RELAY_LAG < T:
            relay(n - RELAY_LAG)
        if 0 <= n - DIAGONAL_LAG < T:
            diagonal(n - DIAGONAL_LAG)
    for t in range(T):
        rest(t)


    def drain(h, c):
        for i in range(1, N):
            a2a_send(h, lax.rem(s + i, N)).wait_send()
        for i, j in peers:
            gather(h, lax.rem(x + j, 2), row_at(i)).wait_send()
        return c

    lax.fori_loop(0, CH, drain, 0)

    def drain_units(t, c):
        swap(t).wait_send()
        to_inner(t).wait_send()

        @pl.when(has_outer)
        def _():
            to_outer(t).wait_send()

        return c

    lax.fori_loop(0, T, drain_units, 0)
    for c in done:
        c.wait_send()


def expand(T, m_in, ag_ref, m_out, re_out, im_out, re_buf, im_buf, sems, m_sem):
    width = re_buf.shape[1]
    half = PANELS // 2
    keep = pltpu.make_async_copy(m_in, m_out, m_sem)
    keep.start()

    def unit(n):
        chip = n // (2 * T)
        v = lax.rem(n, 2 * T)
        low = v < T
        value = ag_ref[2 * chip + jnp.where(low, 0, 1), jnp.where(low, T - 1 - v, v - T)]
        return value.astype(jnp.float32)

    def pair(u):
        return jnp.concatenate([unit(2 * u), unit(2 * u + 1)], axis=0)

    def writes(k, slot):
        at = pl.ds(pl.multiple_of(k * width, width), width)
        return (
            pltpu.make_async_copy(re_buf.at[k], re_out.at[at], sems.at[0, k]),
            pltpu.make_async_copy(im_buf.at[k], im_out.at[at], sems.at[1, k]),
        )

    def one(k, c):
        for d in range(PANELS):
            q = lax.rem(k + d, PANELS)
            at = pl.ds(pl.multiple_of(q * width, width), width)
            if d < half:
                v = pair(PANELS * d + k)
                re, im = v[:, :width], v[:, width:]
            elif d == half:
                v = pair(PANELS * half + jnp.minimum(k, q))
                re, im = v[:, :width], v[:, width:]
                re, im = jnp.where(k < half, re, re.T), jnp.where(k < half, im, -im.T)
            else:
                v = pair(PANELS * (PANELS - d) + q)
                re, im = v[:, :width].T, -v[:, width:].T
            re_buf[k, :, at] = re
            im_buf[k, :, at] = im
        for copy in writes(k, k):
            copy.start()
        return c

    lax.fori_loop(0, PANELS, one, 0)

    def finish(k, c):
        for copy in writes(k, k):
            copy.wait()
        return c

    lax.fori_loop(0, PANELS, finish, 0)
    keep.wait()


def local(N, R, solutions):
    shifts, parts, height, width = solutions.shape
    rows = height // N
    T = units_per_core(R)
    G = 4 * R
    cut = width // 2
    inputs = shifts * parts
    part = 16 if rows % 16 == 0 else rows
    chunks = rows // part
    factor = 1.0 / math.sqrt(height * R)
    w = jnp.asarray(coefficients(shifts * N, N))
    bf, dma = jnp.bfloat16, pltpu.SemaphoreType.DMA
    vmem = pl.BlockSpec(memory_space=pltpu.VMEM)
    hbm = pl.BlockSpec(memory_space=pltpu.HBM)
    unit = (T, cut, 2 * width)
    spreads = T * (1 + (R - 1) + 1 + (R - 1) + 1 + (R - 1) + (R - 1))
    moments, parts_of_gram = pl.pallas_call(
        functools.partial(exchange, N, R, rows, part, T, factor),
        out_shape=(
            jax.ShapeDtypeStruct((OUTS, rows, width), bf),
            jax.ShapeDtypeStruct((G,) + unit, bf),
        ),
        in_specs=[hbm, hbm],
        out_specs=(vmem, vmem),
        scratch_shapes=[
            pltpu.SMEM(w.shape, jnp.float32),
            pltpu.VMEM((inputs, height, width), bf),
            pltpu.VMEM((chunks, N, inputs, part, width), bf),
            pltpu.VMEM((chunks, 2 * R, OUTS, part, width), bf),
            pltpu.VMEM(unit, jnp.float32),
            pltpu.VMEM(unit, bf), pltpu.VMEM(unit, bf), pltpu.VMEM(unit, bf),
            pltpu.VMEM(unit, bf), pltpu.VMEM(unit, bf),
            dma((2,)),
            dma((chunks, N)), dma((chunks, N)), dma((chunks, 2 * R)), dma((chunks, 2 * R)),
            dma((T,)), dma((T,)), dma((T,)), dma((T,)), dma((T,)), dma((T,)),
            dma((spreads,)), dma((T, G)),
        ],
        compiler_params=pltpu.CompilerParams(
            collective_id=0, has_side_effects=True, vmem_limit_bytes=32 * 2**20
        ),
        cost_estimate=pl.CostEstimate(flops=10**9, bytes_accessed=2**23, transcendentals=0),
    )(pltpu.with_memory_space_constraint(w, pltpu.HBM), pltpu.with_memory_space_constraint(solutions.reshape(inputs, height, width), pltpu.HBM))
    size = PANELS * width
    anywhere = pl.BlockSpec(memory_space=pl.ANY)
    moments, gram_real, gram_imag = pl.pallas_call(
        functools.partial(expand, T),
        out_shape=(
            jax.ShapeDtypeStruct((OUTS, rows, width), bf),
            jax.ShapeDtypeStruct((size, size), jnp.float32),
            jax.ShapeDtypeStruct((size, size), jnp.float32),
        ),
        in_specs=[vmem, vmem],
        out_specs=(anywhere, anywhere, anywhere),
        scratch_shapes=[
            pltpu.VMEM((PANELS, width, size), jnp.float32),
            pltpu.VMEM((PANELS, width, size), jnp.float32),
            dma((2, PANELS)),
            dma,
        ],
        compiler_params=pltpu.CompilerParams(vmem_limit_bytes=32 * 2**20),
        cost_estimate=pl.CostEstimate(flops=10**7, bytes_accessed=2**24, transcendentals=0),
    )(moments, parts_of_gram)
    return moments.reshape(2, PANELS, rows, width), gram_real, gram_imag


def solution(mesh):
    return jax.shard_map(
        functools.partial(local, mesh.shape["shift"], mesh.shape["row"]),
        mesh=mesh,
        in_specs=(P("shift", None, "row", None),),
        out_specs=(P(None, None, ("row", "shift"), None), P(), P()),
        check_vma=False,
    )
```

```python
import functools
import math

import jax
import jax.numpy as jnp
import numpy as np
from jax import lax
from jax.experimental import pallas as pl
from jax.experimental.pallas import tpu as pltpu
from jax.sharding import PartitionSpec as P

PANELS = 8
UNITS = PANELS * PANELS
OUTS = 2 * PANELS
RELAY_LAG = 4
DIAGONAL_LAG = 7
MESH = pl.DeviceIdType.MESH


def coefficients(all_shifts, owners):
    indices = np.arange(all_shifts, dtype=np.float32)
    orders = np.arange(1, PANELS + 1, dtype=np.float32)
    step = (np.float32(2.0 * math.pi) * (indices + np.float32(0.5)) / np.float32(all_shifts)).astype(np.float32)
    angles = (orders[:, None] * step[None, :]).astype(np.float32).astype(np.float64)
    cos_part = np.cos(angles).astype(np.float32) / np.float32(all_shifts)
    sin_part = np.sin(angles).astype(np.float32) / np.float32(all_shifts)
    real_row = np.stack([cos_part, -sin_part], axis=-1)
    imag_row = np.stack([sin_part, cos_part], axis=-1)
    both = np.stack([real_row, imag_row], axis=0).reshape(OUTS, owners, -1)
    return both.transpose(1, 0, 2).reshape(-1).astype(jnp.bfloat16).astype(np.float32)


def unit_place(n):
    k = n // PANELS
    kind = lax.rem(n, PANELS)
    left = jnp.where(kind == 0, k // 2, k)
    apart = jnp.where(kind == 0, PANELS // 2, jnp.where(kind == 1, 0, kind // 2))
    half = jnp.where(kind == 0, lax.rem(k, 2), lax.rem(kind, 2))
    return kind, left, lax.rem(left + apart, PANELS), half


def on_or_above(width):
    i = lax.broadcasted_iota(jnp.int32, (width, width), 0)
    j = lax.broadcasted_iota(jnp.int32, (width, width), 1)
    return i, j


def exchange(
    N, R, rows, part, T, factor,
    w_hbm, x_hbm, m_ref, ag,
    w_ref, x_ref, xs, sbuf, own, dout, din, fo, up, fm,
    in_sems, a2a_s, a2a_r, sg_s, sg_x, sg_r, dd_s, dd_r, up_s, fo_r, out_s, in_r, ag_s, near_r, far_r, rest_r,
):
    Z = N // 4
    CH = rows // part
    s = lax.axis_index("shift")
    r = lax.axis_index("row")
    core = lax.rem(s, 2)
    z = s // 4
    x = lax.rem(s // 2, 2)
    inputs = x_ref.shape[0]
    width = x_ref.shape[2]
    cut = width // 2
    slots = 2 * R
    G = 4 * R

    def member(x_, r_, c_):
        return (r_ * 2 + x_) * 2 + c_

    def place(z_, x_, c_):
        return (z_ * 2 + x_) * 2 + c_

    p = member(x, r, core)
    here = r * 2 + x
    partner = place(z, x, 1 - core)
    across = place(z, 1 - x, core)

    def row_at(i):
        return lax.rem(r + i + R, R)

    def remote(src, dst, ss, rr, to_s, to_r):
        return pltpu.make_async_remote_copy(
            src_ref=src, dst_ref=dst, send_sem=ss, recv_sem=rr,
            device_id={"shift": to_s, "row": to_r}, device_id_type=MESH,
        )

    def arrived(ref, sem):
        remote(ref, ref, a2a_s, sem, s, r).wait_recv()

    def left(ref, sem):
        remote(ref, ref, sem, rest_r, s, r).wait_send()

    load_x = pltpu.make_async_copy(x_hbm, x_ref, in_sems.at[0])
    load_w = pltpu.make_async_copy(w_hbm, w_ref, in_sems.at[1])
    load_x.start()
    load_w.start()
    barrier = pltpu.get_barrier_semaphore()
    for i in range(1, N):
        pl.semaphore_signal(barrier, inc=1, device_id={"shift": lax.rem(s + i, N), "row": r}, device_id_type=MESH)
    for i in range(1, R):
        for to in (s, across):
            pl.semaphore_signal(barrier, inc=1, device_id={"shift": to, "row": row_at(i)}, device_id_type=MESH)
    load_x.wait()
    load_w.wait()
    pl.semaphore_wait(barrier, N - 1 + 2 * (R - 1))


    def rows_of(owner, h):
        return pl.ds(pl.multiple_of(owner * rows + h * part, part), part)

    def send_rows(h, to):
        slot = lax.rem(to - s + N, N) - 1
        remote(x_ref.at[:, rows_of(to, h), :], xs.at[h, slot], a2a_s, a2a_r.at[h], to, r).start()

    def send_chunk(h, c):
        for e in range(Z // 2):
            for to_z in (e, Z - 1 - e):
                for dx, dc in ((0, 0), (1, 0), (0, 1), (1, 1)):
                    to = place(to_z, lax.rem(x + dx, 2), lax.rem(core + dc, 2))
                    if dx or dc:
                        send_rows(h, to)
                    else:
                        @pl.when(to_z != z)
                        def _():
                            send_rows(h, to)
        return c

    lax.fori_loop(0, CH, send_chunk, 0)


    def weigh(acc, blocks, source):
        parts = [b.astype(jnp.float32) for b in blocks]
        out = []
        for o in range(OUTS):
            base = (source * OUTS + o) * inputs
            total = parts[0] * w_ref[base]
            for c in range(1, inputs):
                total += parts[c] * w_ref[base + c]
            out.append(total if acc is None else acc[o] + total)
        return tuple(out)

    def panels_to(h, slot, sem, to_s, to_r):
        remote(sbuf.at[h, slot], sbuf.at[h, slot], sg_s, sem, to_s, to_r).start()

    def moments_of(h, c):
        acc = weigh(None, [x_ref[q, rows_of(s, h), :] for q in range(inputs)], s)
        arrived(xs.at[h], a2a_r.at[h])

        def take(j, acc):
            return weigh(acc, [xs[h, j, q] for q in range(inputs)], lax.rem(s - 1 - j + N, N))

        acc = lax.fori_loop(0, N - 1, take, acc)
        at = pl.ds(pl.multiple_of(h * part, part), part)
        for o in range(OUTS):
            value = acc[o].astype(jnp.bfloat16)
            sbuf[h, here, o] = value
            m_ref[o, at, :] = value
        panels_to(h, here, sg_x.at[h], across, r)
        for i in range(1, R):
            panels_to(h, here, sg_r, s, row_at(i))
        return c

    def relay_panels(h):
        slot = r * 2 + 1 - x
        arrived(sbuf.at[h, slot], sg_x.at[h])
        for i in range(1, R):
            panels_to(h, slot, sg_r, s, row_at(i))

    def moments_and_relay(h, c):
        moments_of(h, c)
        relay_panels(h)
        return c

    lax.fori_loop(0, CH - 1, moments_and_relay, 0)
    moments_of(CH - 1, 0)
    for i in range(1, R):
        panels_to(CH - 1, here, sg_r, across, row_at(i))
    arrived(sbuf.at[CH - 1, 0], sg_x.at[CH - 1])
    arrived(sbuf.at[:, pl.ds(0, slots - 2)], sg_r)


    depth = slots * rows
    dims = (((0,), (0,)), ((), ()))

    def panel(k):
        return jnp.concatenate(
            [sbuf[:, :, k].reshape(depth, width), sbuf[:, :, PANELS + k].reshape(depth, width)], axis=1
        )

    def product(a, b):
        v = lax.dot_general(a, b, dims, preferred_element_type=jnp.float32) * factor
        return v[:width, :width] + v[width:, width:], v[:width, width:] - v[width:, :width]

    def halves(re, im):
        return [jnp.concatenate([re[h], im[h]], axis=1) for h in (slice(0, cut), slice(cut, width))]

    def packed(re, im):
        i, j = on_or_above(width)
        v = jnp.where(i <= j, re, im)
        return jnp.concatenate([v[:cut], v[cut:]], axis=1)

    def swap(t):
        return remote(dout.at[t], din.at[t], dd_s, dd_r.at[t], partner, r)

    def give(t, value):
        dout[t] = value.astype(jnp.bfloat16)
        swap(t).start()

    other = member(x, r, 1 - core)
    if T == PANELS:
        low, high = halves(*product(panel(here), panel(here + PANELS // 2)))
        give(0, jnp.where(core == 0, high, low))
        own[0] = jnp.where(core == 0, low, high)
        a = panel(other)
        give(1, packed(*product(a, a)))
        for d in range(1, PANELS // 2):
            low, high = halves(*product(a, panel(lax.rem(other + d, PANELS))))
            give(2 * d, low)
            give(2 * d + 1, high)
        a = panel(p)
        own[1] = packed(*product(a, a))
        for d in range(1, PANELS // 2):
            own[2 * d], own[2 * d + 1] = halves(*product(a, panel(lax.rem(p + d, PANELS))))
    else:
        def unit(n):
            kind, k, q, half = unit_place(n)
            re, im = product(panel(k), panel(q))
            low, high = halves(re, im)
            return jnp.where(kind == 1, packed(re, im), jnp.where(half == 0, low, high))

        def theirs(t, c):
            give(t, unit(other * T + t))
            return c

        def mine(t, c):
            own[t] = unit(p * T + t)
            return c

        lax.fori_loop(0, T, theirs, 0)
        lax.fori_loop(0, T, mine, 0)


    lower = z < Z // 2
    inner = jnp.where(lower, z + 1, z - 1)
    outer = jnp.where(lower, z - 1, z + 1)
    from_end = jnp.where(lower, z, Z - 1 - z)
    is_middle = from_end == Z // 2 - 1
    has_outer = from_end > 0
    inner_s = place(inner, x, core)
    outer_s = place(jnp.where(has_outer, outer, inner), x, core)

    def climb(t, c):
        arrived(din.at[t], dd_r.at[t])
        own[t] = own[t] + din[t].astype(jnp.float32)

        @pl.when(has_outer)
        def _():
            arrived(fo.at[t], fo_r.at[t])
            own[t] = own[t] + fo[t].astype(jnp.float32)

        up[t] = own[t].astype(jnp.bfloat16)

        @pl.when(is_middle)
        def _():
            remote(up.at[t], fm.at[t], up_s, in_r.at[t], inner_s, r).start()

        @pl.when(jnp.logical_not(is_middle))
        def _():
            remote(up.at[t], fo.at[t], up_s, fo_r.at[t], inner_s, r).start()

        return c

    lax.fori_loop(0, T, climb, 0)


    def forward(t, slot, sem, to_s, to_r):
        remote(ag.at[slot, t], ag.at[slot, t], ag_s, sem, to_s, to_r).start()

    def total(t):
        @pl.when(is_middle)
        def _():
            arrived(fm.at[t], in_r.at[t])
            ag[p, t] = (up[t].astype(jnp.float32) + fm[t].astype(jnp.float32)).astype(jnp.bfloat16)

        @pl.when(jnp.logical_not(is_middle))
        def _():
            arrived(ag.at[p, t], in_r.at[t])

        @pl.when(has_outer)
        def _():
            remote(ag.at[p, t], ag.at[p, t], out_s, in_r.at[t], outer_s, r).start()

    def spread(t):
        forward(t, p, near_r.at[t], across, r)
        for i in range(1, R):
            forward(t, p, near_r.at[t], s, row_at(i))
        forward(t, p, rest_r, partner, r)

    def relay(t):
        arrived(ag.at[pl.ds(0, R), t], near_r.at[t])
        first = core == 0
        for i in range(1, R):
            slot = jnp.where(first, member(1 - x, r, core), member(x, row_at(-i), core))
            forward(t, slot, far_r.at[t], jnp.where(first, s, across), jnp.where(first, row_at(i), r))
        forward(t, member(1 - x, r, core), rest_r, partner, r)
        for i in range(1, R):
            forward(t, member(x, row_at(-i), core), rest_r, partner, r)

    def diagonal(t):
        arrived(ag.at[pl.ds(0, R - 1), t], far_r.at[t])
        for i in range(1, R):
            forward(t, member(1 - x, row_at(-i), core), rest_r, partner, r)

    for n in range(T + DIAGONAL_LAG):
        if n < T:
            total(n)
            spread(n)
        if 0 <= n - RELAY_LAG < T:
            relay(n - RELAY_LAG)
        if 0 <= n - DIAGONAL_LAG < T:
            diagonal(n - DIAGONAL_LAG)
    arrived(ag.at[pl.ds(0, slots)], rest_r)


    left(xs, a2a_s)
    left(sbuf.at[:, pl.ds(0, slots - 1)], sg_s)
    left(dout, dd_s)
    left(up, up_s)

    @pl.when(has_outer)
    def _():
        left(up, out_s)

    left(ag.at[pl.ds(0, G - 1)], ag_s)


def expand(T, m_in, ag_ref, m_out, re_out, im_out, re_buf, im_buf, sems, m_sem):
    width = re_buf.shape[1]
    half = PANELS // 2
    keep = pltpu.make_async_copy(m_in, m_out, m_sem)
    keep.start()

    def unit(n):
        return ag_ref[n // T, lax.rem(n, T)].astype(jnp.float32)

    def pair(k, d):
        v = jnp.concatenate([unit(PANELS * k + 2 * d), unit(PANELS * k + 2 * d + 1)], axis=0)
        return v[:, :width], v[:, width:]

    def writes(k, slot):
        at = pl.ds(pl.multiple_of(k * width, width), width)
        return (
            pltpu.make_async_copy(re_buf.at[k], re_out.at[at], sems.at[0, k]),
            pltpu.make_async_copy(im_buf.at[k], im_out.at[at], sems.at[1, k]),
        )

    def one(k, c):
        for d in range(PANELS):
            q = lax.rem(k + d, PANELS)
            at = pl.ds(pl.multiple_of(q * width, width), width)
            if d == 0:
                v = unit(PANELS * k + 1)
                v = jnp.concatenate([v[:, :width], v[:, width:]], axis=0)
                i, j = on_or_above(width)
                re = jnp.where(i <= j, v, v.T)
                im = jnp.where(i > j, v, jnp.where(i < j, -v.T, 0.0))
            elif d < half:
                re, im = pair(k, d)
            elif d == half:
                first = jnp.minimum(k, q)
                v = jnp.concatenate([unit(2 * PANELS * first), unit(2 * PANELS * first + PANELS)], axis=0)
                re, im = v[:, :width], v[:, width:]
                re, im = jnp.where(k < half, re, re.T), jnp.where(k < half, im, -im.T)
            else:
                re, im = pair(q, PANELS - d)
                re, im = re.T, -im.T
            re_buf[k, :, at] = re
            im_buf[k, :, at] = im
        for copy in writes(k, k):
            copy.start()
        return c

    lax.fori_loop(0, PANELS, one, 0)

    def finish(k, c):
        for copy in writes(k, k):
            copy.wait()
        return c

    lax.fori_loop(0, PANELS, finish, 0)
    keep.wait()


def local(N, R, solutions):
    shifts, parts, height, width = solutions.shape
    rows = height // N
    G = 4 * R
    T = UNITS // G
    assert T * G == UNITS
    cut = width // 2
    inputs = shifts * parts
    part = 16 if rows % 16 == 0 else rows
    chunks = rows // part
    factor = 1.0 / math.sqrt(height * R)
    w = jnp.asarray(coefficients(shifts * N, N))
    bf, dma = jnp.bfloat16, pltpu.SemaphoreType.DMA
    vmem = pl.BlockSpec(memory_space=pltpu.VMEM)
    hbm = pl.BlockSpec(memory_space=pltpu.HBM)
    unit = (T, cut, 2 * width)
    moments, parts_of_gram = pl.pallas_call(
        functools.partial(exchange, N, R, rows, part, T, factor),
        out_shape=(
            jax.ShapeDtypeStruct((OUTS, rows, width), bf),
            jax.ShapeDtypeStruct((G,) + unit, bf),
        ),
        in_specs=[hbm, hbm],
        out_specs=(vmem, vmem),
        scratch_shapes=[
            pltpu.SMEM(w.shape, jnp.float32),
            pltpu.VMEM((inputs, height, width), bf),
            pltpu.VMEM((chunks, N - 1, inputs, part, width), bf),
            pltpu.VMEM((chunks, 2 * R, OUTS, part, width), bf),
            pltpu.VMEM(unit, jnp.float32),
            pltpu.VMEM(unit, bf), pltpu.VMEM(unit, bf), pltpu.VMEM(unit, bf),
            pltpu.VMEM(unit, bf), pltpu.VMEM(unit, bf),
            dma((2,)),
            dma, dma((chunks,)), dma, dma((chunks,)), dma,
            dma, dma((T,)), dma, dma((T,)), dma, dma((T,)),
            dma, dma((T,)), dma((T,)), dma,
        ],
        compiler_params=pltpu.CompilerParams(
            collective_id=0, has_side_effects=True, vmem_limit_bytes=32 * 2**20
        ),
        cost_estimate=pl.CostEstimate(flops=10**9, bytes_accessed=2**23, transcendentals=0),
    )(
        pltpu.with_memory_space_constraint(w, pltpu.HBM),
        pltpu.with_memory_space_constraint(solutions.reshape(inputs, height, width), pltpu.HBM),
    )
    size = PANELS * width
    anywhere = pl.BlockSpec(memory_space=pl.ANY)
    moments, gram_real, gram_imag = pl.pallas_call(
        functools.partial(expand, T),
        out_shape=(
            jax.ShapeDtypeStruct((OUTS, rows, width), bf),
            jax.ShapeDtypeStruct((size, size), jnp.float32),
            jax.ShapeDtypeStruct((size, size), jnp.float32),
        ),
        in_specs=[vmem, vmem],
        out_specs=(anywhere, anywhere, anywhere),
        scratch_shapes=[
            pltpu.VMEM((PANELS, width, size), jnp.float32),
            pltpu.VMEM((PANELS, width, size), jnp.float32),
            dma((2, PANELS)),
            dma,
        ],
        compiler_params=pltpu.CompilerParams(vmem_limit_bytes=32 * 2**20),
        cost_estimate=pl.CostEstimate(flops=10**7, bytes_accessed=2**24, transcendentals=0),
    )(moments, parts_of_gram)
    return moments.reshape(2, PANELS, rows, width), gram_real, gram_imag


def solution(mesh):
    return jax.shard_map(
        functools.partial(local, mesh.shape["shift"], mesh.shape["row"]),
        mesh=mesh,
        in_specs=(P("shift", None, "row", None),),
        out_specs=(P(None, None, ("row", "shift"), None), P(), P()),
        check_vma=False,
    )
```

```python
import functools
import math

import jax
import jax.numpy as jnp
import numpy as np
from jax import lax
from jax.experimental import pallas as pl
from jax.experimental.pallas import tpu as pltpu
from jax.sharding import PartitionSpec as P

PANELS = 8
UNITS = PANELS * PANELS
OUTS = 2 * PANELS
CHUNK_ROWS = 16
LEAD = 2
DIRECT = 2
CLOSE_UNITS = 2
SWAP_LAG = 4
RELAY_LAG = 4
DIAGONAL_LAG = 7
MESH = pl.DeviceIdType.MESH


def coefficients(all_shifts, owners):
    indices = np.arange(all_shifts, dtype=np.float32)
    orders = np.arange(1, PANELS + 1, dtype=np.float32)
    step = (np.float32(2.0 * math.pi) * (indices + np.float32(0.5)) / np.float32(all_shifts)).astype(np.float32)
    angles = (orders[:, None] * step[None, :]).astype(np.float32).astype(np.float64)
    cos_part = np.cos(angles).astype(np.float32) / np.float32(all_shifts)
    sin_part = np.sin(angles).astype(np.float32) / np.float32(all_shifts)
    real_row = np.stack([cos_part, -sin_part], axis=-1)
    imag_row = np.stack([sin_part, cos_part], axis=-1)
    both = np.stack([real_row, imag_row], axis=0).reshape(OUTS, owners, -1)
    return both.transpose(1, 0, 2).reshape(-1).astype(jnp.bfloat16).astype(np.float32)


def unit_place(n):
    k = n // PANELS
    kind = lax.rem(n, PANELS)
    left = jnp.where(kind == 0, k // 2, k)
    apart = jnp.where(kind == 0, PANELS // 2, jnp.where(kind == 1, 0, kind // 2))
    half = jnp.where(kind == 0, lax.rem(k, 2), lax.rem(kind, 2))
    return kind, left, lax.rem(left + apart, PANELS), half


def on_or_above(width):
    i = lax.broadcasted_iota(jnp.int32, (width, width), 0)
    j = lax.broadcasted_iota(jnp.int32, (width, width), 1)
    return i, j


def exchange(
    N, R, rows, part, T, factor,
    w_hbm, x_hbm, m_ref, ag,
    w_ref, x_ref, xs, sbuf, own, dout, din, fo, up, fm,
    in_sems, a2a_s, a2a_r, sg_s, sg_x, sg_r, sg_last, dd_s, dd_r, up_s, fo_r, out_s, in_r, ag_s, near_r, far_r, rest_r,
):
    Z = N // 4
    CH = rows // part
    s = lax.axis_index("shift")
    r = lax.axis_index("row")
    core = lax.rem(s, 2)
    z = s // 4
    x = lax.rem(s // 2, 2)
    inputs = x_ref.shape[0]
    width = x_ref.shape[2]
    cut = width // 2
    slots = 2 * R
    G = 4 * R

    def member(x_, r_, c_):
        return (r_ * 2 + x_) * 2 + c_

    def place(z_, x_, c_):
        return (z_ * 2 + x_) * 2 + c_

    p = member(x, r, core)
    here = r * 2 + x
    partner = place(z, x, 1 - core)
    across = place(z, 1 - x, core)

    def row_at(i):
        return lax.rem(r + i + R, R)

    def remote(src, dst, ss, rr, to_s, to_r):
        return pltpu.make_async_remote_copy(
            src_ref=src, dst_ref=dst, send_sem=ss, recv_sem=rr,
            device_id={"shift": to_s, "row": to_r}, device_id_type=MESH,
        )

    def arrived(ref, sem):
        remote(ref, ref, a2a_s, sem, s, r).wait_recv()

    def left(ref, sem):
        remote(ref, ref, sem, rest_r, s, r).wait_send()

    load_x = pltpu.make_async_copy(x_hbm, x_ref, in_sems.at[0])
    load_w = pltpu.make_async_copy(w_hbm, w_ref, in_sems.at[1])
    load_x.start()
    load_w.start()
    barrier = pltpu.get_barrier_semaphore()
    for i in range(1, N):
        pl.semaphore_signal(barrier, inc=1, device_id={"shift": lax.rem(s + i, N), "row": r}, device_id_type=MESH)
    for i in range(1, R):
        for to in (s, across):
            pl.semaphore_signal(barrier, inc=1, device_id={"shift": to, "row": row_at(i)}, device_id_type=MESH)
    load_x.wait()
    load_w.wait()
    pl.semaphore_wait(barrier, N - 1 + 2 * (R - 1))


    def rows_of(owner, h):
        return pl.ds(pl.multiple_of(owner * rows + h * part, part), part)

    def send_rows(h, to):
        slot = lax.rem(to - s + N, N) - 1
        remote(x_ref.at[:, rows_of(to, h), :], xs.at[h, slot], a2a_s, a2a_r.at[h], to, r).start()

    def send_chunk(h, c):
        for e in range(Z // 2):
            for to_z in (e, Z - 1 - e):
                for dx, dc in ((0, 0), (1, 0), (0, 1), (1, 1)):
                    to = place(to_z, lax.rem(x + dx, 2), lax.rem(core + dc, 2))
                    if dx or dc:
                        send_rows(h, to)
                    else:
                        @pl.when(to_z != z)
                        def _():
                            send_rows(h, to)
        return c

    lax.fori_loop(0, min(LEAD, CH), send_chunk, 0)


    def weigh(acc, blocks, source):
        parts = [b.astype(jnp.float32) for b in blocks]
        out = []
        for o in range(OUTS):
            base = (source * OUTS + o) * inputs
            total = parts[0] * w_ref[base]
            for c in range(1, inputs):
                total += parts[c] * w_ref[base + c]
            out.append(total if acc is None else acc[o] + total)
        return tuple(out)

    def panels_to(h, slot, sem, to_s, to_r):
        remote(sbuf.at[h, slot], sbuf.at[h, slot], sg_s, sem, to_s, to_r).start()

    def moments_of(h, c, direct):
        acc = weigh(None, [x_ref[q, rows_of(s, h), :] for q in range(inputs)], s)
        arrived(xs.at[h], a2a_r.at[h])

        @pl.when(h + LEAD < CH)
        def _():
            send_chunk(h + LEAD, 0)

        def take(j, acc):
            return weigh(acc, [xs[h, j, q] for q in range(inputs)], lax.rem(s - 1 - j + N, N))

        acc = lax.fori_loop(0, N - 1, take, acc)
        at = pl.ds(pl.multiple_of(h * part, part), part)
        for o in range(OUTS):
            value = acc[o].astype(jnp.bfloat16)
            sbuf[h, here, o] = value
            m_ref[o, at, :] = value
        if direct:
            for i in range(1, R):
                panels_to(h, here, sg_r, across, row_at(i))
        panels_to(h, here, sg_last if direct else sg_x.at[h], across, r)
        for i in range(1, R):
            panels_to(h, here, sg_r, s, row_at(i))

    def relay_panels(h):
        slot = r * 2 + 1 - x
        arrived(sbuf.at[h, slot], sg_x.at[h])
        for i in range(1, R):
            panels_to(h, slot, sg_r, s, row_at(i))

    def moments_and_relay(h, c):
        moments_of(h, c, False)
        relay_panels(h)
        return c

    last = max(CH - DIRECT, 0)
    lax.fori_loop(0, last, moments_and_relay, 0)

    def moments_direct(h, c):
        moments_of(h, c, True)
        return c

    lax.fori_loop(last, CH, moments_direct, 0)
    arrived(sbuf.at[pl.ds(last, CH - last), 0], sg_last)
    arrived(sbuf.at[:, pl.ds(0, slots - 2)], sg_r)


    depth = slots * rows
    dims = (((0,), (0,)), ((), ()))

    def panel(k):
        return jnp.concatenate(
            [sbuf[:, :, k].reshape(depth, width), sbuf[:, :, PANELS + k].reshape(depth, width)], axis=1
        )

    def product(a, b):
        v = lax.dot_general(a, b, dims, preferred_element_type=jnp.float32)
        return v[:width, :width] + v[width:, width:], v[:width, width:] - v[width:, :width]

    def halves(re, im):
        return [jnp.concatenate([re[h], im[h]], axis=1) for h in (slice(0, cut), slice(cut, width))]

    def packed(re, im):
        i, j = on_or_above(width)
        v = jnp.where(i <= j, re, im)
        return jnp.concatenate([v[:cut], v[cut:]], axis=1)

    def swap(t):
        return remote(dout.at[t], din.at[t], dd_s, dd_r.at[t], partner, r)

    def give(t, value):
        dout[t] = value.astype(jnp.bfloat16)
        swap(t).start()


    lower = z < Z // 2
    inner = jnp.where(lower, z + 1, z - 1)
    outer = jnp.where(lower, z - 1, z + 1)
    from_end = jnp.where(lower, z, Z - 1 - z)
    is_middle = from_end == Z // 2 - 1
    has_outer = from_end > 0
    inner_s = place(inner, x, core)
    outer_s = place(jnp.where(has_outer, outer, inner), x, core)

    def climb(t, c):
        arrived(din.at[t], dd_r.at[t])
        own[t] = (own[t] + din[t].astype(jnp.float32)) * factor

        @pl.when(has_outer)
        def _():
            arrived(fo.at[t], fo_r.at[t])
            own[t] = own[t] + fo[t].astype(jnp.float32)

        up[t] = own[t].astype(jnp.bfloat16)

        @pl.when(is_middle)
        def _():
            remote(up.at[t], fm.at[t], up_s, in_r.at[t], inner_s, r).start()

        @pl.when(jnp.logical_not(is_middle))
        def _():
            remote(up.at[t], fo.at[t], up_s, fo_r.at[t], inner_s, r).start()

        return c


    def forward(t, slot, sem, to_s, to_r):
        remote(ag.at[slot, t], ag.at[slot, t], ag_s, sem, to_s, to_r).start()

    def total(t):
        @pl.when(is_middle)
        def _():
            arrived(fm.at[t], in_r.at[t])
            ag[p, t] = (up[t].astype(jnp.float32) + fm[t].astype(jnp.float32)).astype(jnp.bfloat16)

        @pl.when(jnp.logical_not(is_middle))
        def _():
            arrived(ag.at[p, t], in_r.at[t])

        @pl.when(has_outer)
        def _():
            remote(ag.at[p, t], ag.at[p, t], out_s, in_r.at[t], outer_s, r).start()

    def close(t):
        return t >= T - CLOSE_UNITS

    def spread(t):
        if close(t):
            for i in range(1, R):
                forward(t, p, far_r.at[t], across, row_at(i))
        forward(t, p, near_r.at[t], across, r)
        for i in range(1, R):
            forward(t, p, near_r.at[t], s, row_at(i))
        forward(t, p, rest_r, partner, r)

    def finish(t):
        total(t)
        spread(t)

    def climb_and_finish(t):
        climb(t, 0)
        if t >= SWAP_LAG:
            @pl.when(is_middle)
            def _():
                finish(t - SWAP_LAG)

    other = member(x, r, 1 - core)
    if T == PANELS:
        low, high = halves(*product(panel(here), panel(here + PANELS // 2)))
        give(0, jnp.where(core == 0, high, low))
        own[0] = jnp.where(core == 0, low, high)
        a = panel(other)
        give(1, packed(*product(a, a)))
        for d in range(1, PANELS // 2):
            low, high = halves(*product(a, panel(lax.rem(other + d, PANELS))))
            give(2 * d, low)
            give(2 * d + 1, high)
        climb_and_finish(0)
        a = panel(p)
        own[1] = packed(*product(a, a))
        climb_and_finish(1)
        for d in range(1, PANELS // 2):
            own[2 * d], own[2 * d + 1] = halves(*product(a, panel(lax.rem(p + d, PANELS))))
            climb_and_finish(2 * d)
            climb_and_finish(2 * d + 1)
    else:
        def unit(n):
            kind, k, q, half = unit_place(n)
            re, im = product(panel(k), panel(q))
            low, high = halves(re, im)
            return jnp.where(kind == 1, packed(re, im), jnp.where(half == 0, low, high))

        def theirs(t, c):
            give(t, unit(other * T + t))
            return c

        def mine(t, c):
            own[t] = unit(p * T + t)
            return c

        lax.fori_loop(0, T, theirs, 0)
        lax.fori_loop(0, T, mine, 0)
        for t in range(T):
            climb_and_finish(t)

    def relay(t):
        arrived(ag.at[pl.ds(0, R), t], near_r.at[t])
        first = core == 0
        for i in range(1, R if not close(t) else 1):
            slot = jnp.where(first, member(1 - x, r, core), member(x, row_at(-i), core))
            forward(t, slot, far_r.at[t], jnp.where(first, s, across), jnp.where(first, row_at(i), r))
        forward(t, member(1 - x, r, core), rest_r, partner, r)
        for i in range(1, R):
            forward(t, member(x, row_at(-i), core), rest_r, partner, r)

    def diagonal(t):
        arrived(ag.at[pl.ds(0, R - 1), t], far_r.at[t])
        for i in range(1, R):
            forward(t, member(1 - x, row_at(-i), core), rest_r, partner, r)

    for n in range(T + DIAGONAL_LAG):
        if n < T - SWAP_LAG:
            @pl.when(jnp.logical_not(is_middle))
            def _():
                finish(n)
        elif n < T:
            finish(n)
        if 0 <= n - RELAY_LAG < T:
            relay(n - RELAY_LAG)
        if 0 <= n - DIAGONAL_LAG < T:
            diagonal(n - DIAGONAL_LAG)
    arrived(ag.at[pl.ds(0, slots)], rest_r)


    left(xs, a2a_s)
    left(sbuf.at[:, pl.ds(0, slots - 1)], sg_s)
    left(dout, dd_s)
    left(up, up_s)

    @pl.when(has_outer)
    def _():
        left(up, out_s)

    left(ag.at[pl.ds(0, G - 1)], ag_s)


def expand(T, m_in, ag_ref, m_out, re_out, im_out, re_buf, im_buf, sems, m_sem):
    width = re_buf.shape[1]
    half = PANELS // 2
    keep = pltpu.make_async_copy(m_in, m_out, m_sem)
    keep.start()

    def unit(n):
        return ag_ref[n // T, lax.rem(n, T)].astype(jnp.float32)

    def pair(k, d):
        v = jnp.concatenate([unit(PANELS * k + 2 * d), unit(PANELS * k + 2 * d + 1)], axis=0)
        return v[:, :width], v[:, width:]

    def writes(k, slot):
        at = pl.ds(pl.multiple_of(k * width, width), width)
        return (
            pltpu.make_async_copy(re_buf.at[k], re_out.at[at], sems.at[0, k]),
            pltpu.make_async_copy(im_buf.at[k], im_out.at[at], sems.at[1, k]),
        )

    def one(k, c):
        for d in range(PANELS):
            q = lax.rem(k + d, PANELS)
            at = pl.ds(pl.multiple_of(q * width, width), width)
            if d == 0:
                v = unit(PANELS * k + 1)
                v = jnp.concatenate([v[:, :width], v[:, width:]], axis=0)
                i, j = on_or_above(width)
                re = jnp.where(i <= j, v, v.T)
                im = jnp.where(i > j, v, jnp.where(i < j, -v.T, 0.0))
            elif d < half:
                re, im = pair(k, d)
            elif d == half:
                first = jnp.minimum(k, q)
                v = jnp.concatenate([unit(2 * PANELS * first), unit(2 * PANELS * first + PANELS)], axis=0)
                re, im = v[:, :width], v[:, width:]
                re, im = jnp.where(k < half, re, re.T), jnp.where(k < half, im, -im.T)
            else:
                re, im = pair(q, PANELS - d)
                re, im = re.T, -im.T
            re_buf[k, :, at] = re
            im_buf[k, :, at] = im
        for copy in writes(k, k):
            copy.start()
        return c

    lax.fori_loop(0, PANELS, one, 0)

    def finish(k, c):
        for copy in writes(k, k):
            copy.wait()
        return c

    lax.fori_loop(0, PANELS, finish, 0)
    keep.wait()


def local(N, R, solutions):
    shifts, parts, height, width = solutions.shape
    rows = height // N
    G = 4 * R
    T = UNITS // G
    assert T * G == UNITS
    cut = width // 2
    inputs = shifts * parts
    part = CHUNK_ROWS if rows % CHUNK_ROWS == 0 else rows
    chunks = rows // part
    factor = 1.0 / math.sqrt(height * R)
    w = jnp.asarray(coefficients(shifts * N, N))
    bf, dma = jnp.bfloat16, pltpu.SemaphoreType.DMA
    vmem = pl.BlockSpec(memory_space=pltpu.VMEM)
    hbm = pl.BlockSpec(memory_space=pltpu.HBM)
    unit = (T, cut, 2 * width)
    moments, parts_of_gram = pl.pallas_call(
        functools.partial(exchange, N, R, rows, part, T, factor),
        out_shape=(
            jax.ShapeDtypeStruct((OUTS, rows, width), bf),
            jax.ShapeDtypeStruct((G,) + unit, bf),
        ),
        in_specs=[hbm, hbm],
        out_specs=(vmem, vmem),
        scratch_shapes=[
            pltpu.SMEM(w.shape, jnp.float32),
            pltpu.VMEM((inputs, height, width), bf),
            pltpu.VMEM((chunks, N - 1, inputs, part, width), bf),
            pltpu.VMEM((chunks, 2 * R, OUTS, part, width), bf),
            pltpu.VMEM(unit, jnp.float32),
            pltpu.VMEM(unit, bf), pltpu.VMEM(unit, bf), pltpu.VMEM(unit, bf),
            pltpu.VMEM(unit, bf), pltpu.VMEM(unit, bf),
            dma((2,)),
            dma, dma((chunks,)), dma, dma((chunks,)), dma, dma,
            dma, dma((T,)), dma, dma((T,)), dma, dma((T,)),
            dma, dma((T,)), dma((T,)), dma,
        ],
        compiler_params=pltpu.CompilerParams(
            collective_id=0, has_side_effects=True, vmem_limit_bytes=32 * 2**20
        ),
        cost_estimate=pl.CostEstimate(flops=10**9, bytes_accessed=2**23, transcendentals=0),
    )(
        pltpu.with_memory_space_constraint(w, pltpu.HBM),
        pltpu.with_memory_space_constraint(solutions.reshape(inputs, height, width), pltpu.HBM),
    )
    size = PANELS * width
    anywhere = pl.BlockSpec(memory_space=pl.ANY)
    moments, gram_real, gram_imag = pl.pallas_call(
        functools.partial(expand, T),
        out_shape=(
            jax.ShapeDtypeStruct((OUTS, rows, width), bf),
            jax.ShapeDtypeStruct((size, size), jnp.float32),
            jax.ShapeDtypeStruct((size, size), jnp.float32),
        ),
        in_specs=[vmem, vmem],
        out_specs=(anywhere, anywhere, anywhere),
        scratch_shapes=[
            pltpu.VMEM((PANELS, width, size), jnp.float32),
            pltpu.VMEM((PANELS, width, size), jnp.float32),
            dma((2, PANELS)),
            dma,
        ],
        compiler_params=pltpu.CompilerParams(vmem_limit_bytes=32 * 2**20),
        cost_estimate=pl.CostEstimate(flops=10**7, bytes_accessed=2**24, transcendentals=0),
    )(moments, parts_of_gram)
    return moments.reshape(2, PANELS, rows, width), gram_real, gram_imag


def solution(mesh):
    return jax.shard_map(
        functools.partial(local, mesh.shape["shift"], mesh.shape["row"]),
        mesh=mesh,
        in_specs=(P("shift", None, "row", None),),
        out_specs=(P(None, None, ("row", "shift"), None), P(), P()),
        check_vma=False,
    )
```

```python
import functools
import math

import jax
import jax.numpy as jnp
import numpy as np
from jax import lax
from jax.experimental import pallas as pl
from jax.experimental.pallas import tpu as pltpu
from jax.sharding import PartitionSpec as P

PANELS = 8
UNITS = PANELS * PANELS
OUTS = 2 * PANELS
CHUNK_ROWS = 16
LEAD = 2
DIRECT = 2
PIECES = 2
CLOSE_PIECES = 4
SWAP_LAG = 8
OVER_Z = (1, 2, 3)
RELAY_LAG = 6
DIAGONAL_LAG = 11
MESH = pl.DeviceIdType.MESH


def coefficients(all_shifts, owners):
    indices = np.arange(all_shifts, dtype=np.float32)
    orders = np.arange(1, PANELS + 1, dtype=np.float32)
    step = (np.float32(2.0 * math.pi) * (indices + np.float32(0.5)) / np.float32(all_shifts)).astype(np.float32)
    angles = (orders[:, None] * step[None, :]).astype(np.float32).astype(np.float64)
    cos_part = np.cos(angles).astype(np.float32) / np.float32(all_shifts)
    sin_part = np.sin(angles).astype(np.float32) / np.float32(all_shifts)
    real_row = np.stack([cos_part, -sin_part], axis=-1)
    imag_row = np.stack([sin_part, cos_part], axis=-1)
    both = np.stack([real_row, imag_row], axis=0).reshape(OUTS, owners, -1)
    return both.transpose(1, 0, 2).reshape(-1).astype(jnp.bfloat16).astype(np.float32)


def unit_place(n):
    k = n // PANELS
    kind = lax.rem(n, PANELS)
    left = jnp.where(kind == 0, k // 2, k)
    apart = jnp.where(kind == 0, PANELS // 2, jnp.where(kind == 1, 0, kind // 2))
    half = jnp.where(kind == 0, lax.rem(k, 2), lax.rem(kind, 2))
    return kind, left, lax.rem(left + apart, PANELS), half


def on_or_above(width):
    i = lax.broadcasted_iota(jnp.int32, (width, width), 0)
    j = lax.broadcasted_iota(jnp.int32, (width, width), 1)
    return i, j


def exchange(
    N, R, rows, part, T, factor,
    w_hbm, x_hbm, m_ref, ag,
    w_ref, x_ref, xs, sbuf, own, dout, din, fo, up, fm,
    in_sems, a2a_s, a2a_r, sg_s, sg_x, sg_r, sg_last, dd_s, dd_r, up_s, fo_r, out_s, in_r, ag_s, near_r, far_r, rest_r, over_s,
):
    Z = N // 4
    CH = rows // part
    s = lax.axis_index("shift")
    r = lax.axis_index("row")
    core = lax.rem(s, 2)
    z = s // 4
    x = lax.rem(s // 2, 2)
    inputs = x_ref.shape[0]
    width = x_ref.shape[2]
    cut = width // 2
    piece = cut // PIECES
    U = T * PIECES
    slots = 2 * R
    G = 4 * R

    def member(x_, r_, c_):
        return (r_ * 2 + x_) * 2 + c_

    def place(z_, x_, c_):
        return (z_ * 2 + x_) * 2 + c_

    p = member(x, r, core)
    here = r * 2 + x
    partner = place(z, x, 1 - core)
    across = place(z, 1 - x, core)

    def row_at(i):
        return lax.rem(r + i + R, R)

    def remote(src, dst, ss, rr, to_s, to_r):
        return pltpu.make_async_remote_copy(
            src_ref=src, dst_ref=dst, send_sem=ss, recv_sem=rr,
            device_id={"shift": to_s, "row": to_r}, device_id_type=MESH,
        )

    def arrived(ref, sem):
        remote(ref, ref, a2a_s, sem, s, r).wait_recv()

    def left(ref, sem):
        remote(ref, ref, sem, rest_r, s, r).wait_send()

    load_x = pltpu.make_async_copy(x_hbm, x_ref, in_sems.at[0])
    load_w = pltpu.make_async_copy(w_hbm, w_ref, in_sems.at[1])
    load_x.start()
    load_w.start()
    barrier = pltpu.get_barrier_semaphore()
    for i in range(1, N):
        pl.semaphore_signal(barrier, inc=1, device_id={"shift": lax.rem(s + i, N), "row": r}, device_id_type=MESH)
    for i in range(1, R):
        for to in (s, across):
            pl.semaphore_signal(barrier, inc=1, device_id={"shift": to, "row": row_at(i)}, device_id_type=MESH)
    load_x.wait()
    load_w.wait()
    pl.semaphore_wait(barrier, N - 1 + 2 * (R - 1))


    def rows_of(owner, h):
        return pl.ds(pl.multiple_of(owner * rows + h * part, part), part)

    def send_rows(h, to):
        slot = lax.rem(to - s + N, N) - 1
        remote(x_ref.at[:, rows_of(to, h), :], xs.at[h, slot], a2a_s, a2a_r.at[h, jnp.where(slot < N // 2, 0, 1)], to, r).start()

    def send_chunk(h, c):
        for e in range(Z // 2):
            for to_z in (e, Z - 1 - e):
                for dx, dc in ((0, 0), (1, 0), (0, 1), (1, 1)):
                    to = place(to_z, lax.rem(x + dx, 2), lax.rem(core + dc, 2))
                    if dx or dc:
                        send_rows(h, to)
                    else:
                        @pl.when(to_z != z)
                        def _():
                            send_rows(h, to)
        return c

    lax.fori_loop(0, min(LEAD, CH), send_chunk, 0)


    def weigh(acc, blocks, source):
        parts = [b.astype(jnp.float32) for b in blocks]
        out = []
        for o in range(OUTS):
            base = (source * OUTS + o) * inputs
            total = parts[0] * w_ref[base]
            for c in range(1, inputs):
                total += parts[c] * w_ref[base + c]
            out.append(total if acc is None else acc[o] + total)
        return tuple(out)

    def panels_to(h, slot, sem, to_s, to_r):
        remote(sbuf.at[h, slot], sbuf.at[h, slot], sg_s, sem, to_s, to_r).start()

    def moments_of(h, c, direct):
        acc = weigh(None, [x_ref[q, rows_of(s, h), :] for q in range(inputs)], s)
        arrived(xs.at[h, pl.ds(0, N // 2)], a2a_r.at[h, 0])

        def take(j, acc):
            return weigh(acc, [xs[h, j, q] for q in range(inputs)], lax.rem(s - 1 - j + N, N))

        acc = lax.fori_loop(0, N // 2, take, acc)
        arrived(xs.at[h, pl.ds(N // 2, N - 1 - N // 2)], a2a_r.at[h, 1])

        @pl.when(h + LEAD < CH)
        def _():
            send_chunk(h + LEAD, 0)

        acc = lax.fori_loop(N // 2, N - 1, take, acc)
        at = pl.ds(pl.multiple_of(h * part, part), part)
        for o in range(OUTS):
            value = acc[o].astype(jnp.bfloat16)
            sbuf[h, here, o] = value
            m_ref[o, at, :] = value
        if direct:
            for i in range(1, R):
                panels_to(h, here, sg_r, across, row_at(i))
        panels_to(h, here, sg_last if direct else sg_x.at[h], across, r)
        for i in range(1, R):
            panels_to(h, here, sg_r, s, row_at(i))

    def relay_panels(h):
        slot = r * 2 + 1 - x
        arrived(sbuf.at[h, slot], sg_x.at[h])
        for i in range(1, R):
            panels_to(h, slot, sg_r, s, row_at(i))

    def moments_and_relay(h, c):
        moments_of(h, c, False)
        relay_panels(h)
        return c

    last = max(CH - DIRECT, 0)
    lax.fori_loop(0, last, moments_and_relay, 0)

    def moments_direct(h, c):
        moments_of(h, c, True)
        return c

    lax.fori_loop(last, CH, moments_direct, 0)
    arrived(sbuf.at[pl.ds(last, CH - last), 0], sg_last)
    arrived(sbuf.at[:, pl.ds(0, slots - 2)], sg_r)


    depth = slots * rows

    def panel(k):
        return jnp.concatenate(
            [sbuf[:, :, k].reshape(depth, width), sbuf[:, :, PANELS + k].reshape(depth, width)], axis=1
        )

    def turned(k):
        return panel(k).T

    def product(a, b):
        v = jnp.dot(a, b, preferred_element_type=jnp.float32)
        return v[:width, :width] + v[width:, width:], v[:width, width:] - v[width:, :width]

    def halves(re, im):
        return [jnp.concatenate([re[h], im[h]], axis=1) for h in (slice(0, cut), slice(cut, width))]

    def packed(re, im):
        i, j = on_or_above(width)
        v = jnp.where(i <= j, re, im)
        return jnp.concatenate([v[:cut], v[cut:]], axis=1)

    def swap(t):
        return remote(dout.at[t], din.at[t], dd_s, dd_r.at[t], partner, r)

    def give(t, value):
        dout[t] = value.astype(jnp.bfloat16)
        swap(t).start()


    lower = z < Z // 2
    inner = jnp.where(lower, z + 1, z - 1)
    outer = jnp.where(lower, z - 1, z + 1)
    from_end = jnp.where(lower, z, Z - 1 - z)
    is_middle = from_end == Z // 2 - 1
    has_outer = from_end > 0
    inner_s = place(inner, x, core)
    outer_s = place(jnp.where(has_outer, outer, inner), x, core)

    def of(u):
        return u // PIECES, slice(u % PIECES * piece, u % PIECES * piece + piece)

    def climb(u):
        t, at = of(u)
        if u % PIECES == 0:
            arrived(din.at[t], dd_r.at[t])
        own[t, at] = (own[t, at] + din[t, at].astype(jnp.float32)) * factor

        @pl.when(has_outer)
        def _():
            arrived(fo.at[t, at], fo_r.at[u])
            own[t, at] = own[t, at] + fo[t, at].astype(jnp.float32)

        up[t, at] = own[t, at].astype(jnp.bfloat16)

        @pl.when(is_middle)
        def _():
            remote(up.at[t, at], fm.at[t, at], up_s, in_r.at[u], inner_s, r).start()

        @pl.when(jnp.logical_not(is_middle))
        def _():
            remote(up.at[t, at], fo.at[t, at], up_s, fo_r.at[u], inner_s, r).start()

    def forward(u, slot, sem, to_s, to_r):
        t, at = of(u)
        remote(ag.at[slot, t, at], ag.at[slot, t, at], ag_s, sem, to_s, to_r).start()

    def total(u):
        t, at = of(u)

        @pl.when(is_middle)
        def _():
            arrived(fm.at[t, at], in_r.at[u])
            ag[p, t, at] = (up[t, at].astype(jnp.float32) + fm[t, at].astype(jnp.float32)).astype(jnp.bfloat16)

        @pl.when(jnp.logical_not(is_middle))
        def _():
            arrived(ag.at[p, t, at], in_r.at[u])

        @pl.when(has_outer)
        def _():
            remote(ag.at[p, t, at], ag.at[p, t, at], out_s, in_r.at[u], outer_s, r).start()

    def close(u):
        return u >= U - CLOSE_PIECES

    over_z = [t for t in OVER_Z if t < T and not close(t * PIECES + PIECES - 1)] if Z > 2 and R > 1 else []

    def spread(u):
        forward(u, p, rest_r, partner, r)
        if close(u):
            for i in range(1, R):
                forward(u, p, far_r.at[u], across, row_at(i))
        ways = [(across, r)] + [(s, row_at(i)) for i in range(1, R)]
        for (to_s, to_r), (other_s, other_r) in zip(ways, reversed(ways)):
            forward(u, p, near_r.at[u], jnp.where(core == 0, to_s, other_s), jnp.where(core == 0, to_r, other_r))

    def finish(u):
        total(u)
        spread(u)

    def climb_and_finish(t):
        for u in range(t * PIECES, (t + 1) * PIECES):
            climb(u)
            if u >= SWAP_LAG:
                pl.when(is_middle)(functools.partial(finish, u - SWAP_LAG))

    other = member(x, r, 1 - core)
    if T == PANELS:
        low, high = halves(*product(turned(here), panel(here + PANELS // 2)))
        give(0, jnp.where(core == 0, high, low))
        own[0] = jnp.where(core == 0, low, high)
        a, b = turned(other), turned(p)
        give(1, packed(*product(a, panel(other))))
        own[1] = packed(*product(b, panel(p)))
        for d in range(1, PANELS // 2):
            low, high = halves(*product(a, panel(lax.rem(other + d, PANELS))))
            give(2 * d, low)
            give(2 * d + 1, high)
            climb_and_finish(2 * d - 2)
            climb_and_finish(2 * d - 1)
            own[2 * d], own[2 * d + 1] = halves(*product(b, panel(lax.rem(p + d, PANELS))))
        climb_and_finish(T - 2)
        climb_and_finish(T - 1)
    else:
        def unit(n):
            kind, k, q, half = unit_place(n)
            re, im = product(turned(k), panel(q))
            low, high = halves(re, im)
            return jnp.where(kind == 1, packed(re, im), jnp.where(half == 0, low, high))

        def theirs(t, c):
            give(t, unit(other * T + t))
            return c

        def mine(t, c):
            own[t] = unit(p * T + t)
            return c

        lax.fori_loop(0, T, theirs, 0)
        lax.fori_loop(0, T, mine, 0)
        for t in range(T):
            climb_and_finish(t)

    def relay(u):
        t, at = of(u)
        arrived(ag.at[pl.ds(0, R), t, at], near_r.at[u])
        forward(u, member(1 - x, r, core), rest_r, partner, r)
        for i in range(1, R):
            forward(u, member(x, row_at(-i), core), rest_r, partner, r)
        first = core == 0

        def to_diagonal():
            for i in range(1, R):
                slot = jnp.where(first, member(1 - x, r, core), member(x, row_at(-i), core))
                forward(u, slot, far_r.at[u], jnp.where(first, s, across), jnp.where(first, row_at(i), r))

        if t in over_z:
            pl.when(has_outer)(to_diagonal)
        elif not close(u):
            to_diagonal()

    def diagonal(u):
        t, at = of(u)
        arrived(ag.at[pl.ds(0, R - 1), t, at], far_r.at[u])
        for i in range(1, R):
            slot = member(1 - x, row_at(-i), core)
            if t in over_z:
                @pl.when(from_end == 1)
                def _():
                    remote(ag.at[slot, t, at], ag.at[slot, t, at], over_s, far_r.at[u], outer_s, r).start()
            forward(u, slot, rest_r, partner, r)

    for n in range(U + DIAGONAL_LAG):
        if n < U - SWAP_LAG:
            pl.when(jnp.logical_not(is_middle))(functools.partial(finish, n))
        elif n < U:
            finish(n)
        if 0 <= n - RELAY_LAG < U:
            relay(n - RELAY_LAG)
        if 0 <= n - DIAGONAL_LAG < U:
            diagonal(n - DIAGONAL_LAG)
    arrived(ag.at[pl.ds(0, slots)], rest_r)


    left(xs, a2a_s)
    left(sbuf.at[:, pl.ds(0, slots - 1)], sg_s)
    left(dout, dd_s)
    left(up, up_s)

    @pl.when(has_outer)
    def _():
        left(up, out_s)

    left(ag.at[pl.ds(0, G - 1), pl.ds(0, T - len(over_z))], ag_s)
    if over_z:
        left(ag.at[pl.ds(0, G - R), pl.ds(0, len(over_z))], ag_s)
        few = ag.at[pl.ds(0, R - 1), pl.ds(0, len(over_z))]

        @pl.when(has_outer)
        def _():
            left(few, ag_s)

        @pl.when(from_end == 1)
        def _():
            left(few, over_s)


def expand(T, m_in, ag_ref, m_out, re_out, im_out, re_buf, im_buf, sems, m_sem):
    width = re_buf.shape[1]
    half = PANELS // 2
    keep = pltpu.make_async_copy(m_in, m_out, m_sem)
    keep.start()

    def unit(n):
        return ag_ref[n // T, lax.rem(n, T)].astype(jnp.float32)

    def pair(k, d):
        v = jnp.concatenate([unit(PANELS * k + 2 * d), unit(PANELS * k + 2 * d + 1)], axis=0)
        return v[:, :width], v[:, width:]

    def writes(k, slot):
        at = pl.ds(pl.multiple_of(k * width, width), width)
        return (
            pltpu.make_async_copy(re_buf.at[k], re_out.at[at], sems.at[0, k]),
            pltpu.make_async_copy(im_buf.at[k], im_out.at[at], sems.at[1, k]),
        )

    def one(k, c):
        for d in range(PANELS):
            q = lax.rem(k + d, PANELS)
            at = pl.ds(pl.multiple_of(q * width, width), width)
            if d == 0:
                v = unit(PANELS * k + 1)
                v = jnp.concatenate([v[:, :width], v[:, width:]], axis=0)
                i, j = on_or_above(width)
                re = jnp.where(i <= j, v, v.T)
                im = jnp.where(i > j, v, jnp.where(i < j, -v.T, 0.0))
            elif d < half:
                re, im = pair(k, d)
            elif d == half:
                first = jnp.minimum(k, q)
                v = jnp.concatenate([unit(2 * PANELS * first), unit(2 * PANELS * first + PANELS)], axis=0)
                re, im = v[:, :width], v[:, width:]
                re, im = jnp.where(k < half, re, re.T), jnp.where(k < half, im, -im.T)
            else:
                re, im = pair(q, PANELS - d)
                re, im = re.T, -im.T
            re_buf[k, :, at] = re
            im_buf[k, :, at] = im
        for copy in writes(k, k):
            copy.start()
        return c

    lax.fori_loop(0, PANELS, one, 0)

    def finish(k, c):
        for copy in writes(k, k):
            copy.wait()
        return c

    lax.fori_loop(0, PANELS, finish, 0)
    keep.wait()


def local(N, R, solutions):
    shifts, parts, height, width = solutions.shape
    rows = height // N
    G = 4 * R
    T = UNITS // G
    assert T * G == UNITS
    cut = width // 2
    inputs = shifts * parts
    part = CHUNK_ROWS if rows % CHUNK_ROWS == 0 else rows
    chunks = rows // part
    factor = 1.0 / math.sqrt(height * R)
    w = jnp.asarray(coefficients(shifts * N, N))
    bf, dma = jnp.bfloat16, pltpu.SemaphoreType.DMA
    vmem = pl.BlockSpec(memory_space=pltpu.VMEM)
    hbm = pl.BlockSpec(memory_space=pltpu.HBM)
    unit = (T, cut, 2 * width)
    moments, parts_of_gram = pl.pallas_call(
        functools.partial(exchange, N, R, rows, part, T, factor),
        out_shape=(
            jax.ShapeDtypeStruct((OUTS, rows, width), bf),
            jax.ShapeDtypeStruct((G,) + unit, bf),
        ),
        in_specs=[hbm, hbm],
        out_specs=(vmem, vmem),
        scratch_shapes=[
            pltpu.SMEM(w.shape, jnp.float32),
            pltpu.VMEM((inputs, height, width), bf),
            pltpu.VMEM((chunks, N - 1, inputs, part, width), bf),
            pltpu.VMEM((chunks, 2 * R, OUTS, part, width), bf),
            pltpu.VMEM(unit, jnp.float32),
            pltpu.VMEM(unit, bf), pltpu.VMEM(unit, bf), pltpu.VMEM(unit, bf),
            pltpu.VMEM(unit, bf), pltpu.VMEM(unit, bf),
            dma((2,)),
            dma, dma((chunks, 2)), dma, dma((chunks,)), dma, dma,
            dma, dma((T,)), dma, dma((T * PIECES,)), dma, dma((T * PIECES,)),
            dma, dma((T * PIECES,)), dma((T * PIECES,)), dma, dma,
        ],
        compiler_params=pltpu.CompilerParams(
            collective_id=0, has_side_effects=True, vmem_limit_bytes=32 * 2**20
        ),
        cost_estimate=pl.CostEstimate(flops=10**9, bytes_accessed=2**23, transcendentals=0),
    )(
        pltpu.with_memory_space_constraint(w, pltpu.HBM),
        pltpu.with_memory_space_constraint(solutions.reshape(inputs, height, width), pltpu.HBM),
    )
    size = PANELS * width
    anywhere = pl.BlockSpec(memory_space=pl.ANY)
    moments, gram_real, gram_imag = pl.pallas_call(
        functools.partial(expand, T),
        out_shape=(
            jax.ShapeDtypeStruct((OUTS, rows, width), bf),
            jax.ShapeDtypeStruct((size, size), jnp.float32),
            jax.ShapeDtypeStruct((size, size), jnp.float32),
        ),
        in_specs=[vmem, vmem],
        out_specs=(anywhere, anywhere, anywhere),
        scratch_shapes=[
            pltpu.VMEM((PANELS, width, size), jnp.float32),
            pltpu.VMEM((PANELS, width, size), jnp.float32),
            dma((2, PANELS)),
            dma,
        ],
        compiler_params=pltpu.CompilerParams(vmem_limit_bytes=32 * 2**20),
        cost_estimate=pl.CostEstimate(flops=10**7, bytes_accessed=2**24, transcendentals=0),
    )(moments, parts_of_gram)
    return moments.reshape(2, PANELS, rows, width), gram_real, gram_imag


def solution(mesh):
    return jax.shard_map(
        functools.partial(local, mesh.shape["shift"], mesh.shape["row"]),
        mesh=mesh,
        in_specs=(P("shift", None, "row", None),),
        out_specs=(P(None, None, ("row", "shift"), None), P(), P()),
        check_vma=False,
    )
```

```python
import functools
import math

import jax
import jax.numpy as jnp
import numpy as np
from jax import lax
from jax.experimental import pallas as pl
from jax.experimental.pallas import tpu as pltpu
from jax.sharding import PartitionSpec as P

PANELS = 8
UNITS = PANELS * PANELS
OUTS = 2 * PANELS
CHUNK_ROWS = 16
LEAD = 2
PIECES = 2
CLOSE_PIECES = 4
SWAP_LAG = 8
OVER_Z = (1, 2, 3)
RELAY_LAG = 6
DIAGONAL_LAG = 11
MESH = pl.DeviceIdType.MESH


def coefficients(all_shifts, owners):
    indices = np.arange(all_shifts, dtype=np.float32)
    orders = np.arange(1, PANELS + 1, dtype=np.float32)
    step = (np.float32(2.0 * math.pi) * (indices + np.float32(0.5)) / np.float32(all_shifts)).astype(np.float32)
    angles = (orders[:, None] * step[None, :]).astype(np.float32).astype(np.float64)
    cos_part = np.cos(angles).astype(np.float32) / np.float32(all_shifts)
    sin_part = np.sin(angles).astype(np.float32) / np.float32(all_shifts)
    real_row = np.stack([cos_part, -sin_part], axis=-1)
    imag_row = np.stack([sin_part, cos_part], axis=-1)
    both = np.stack([real_row, imag_row], axis=0).reshape(OUTS, owners, -1)
    return both.transpose(1, 0, 2).reshape(-1).astype(jnp.bfloat16).astype(np.float32)


def unit_place(n):
    k = n // PANELS
    kind = lax.rem(n, PANELS)
    left = jnp.where(kind == 0, k // 2, k)
    apart = jnp.where(kind == 0, PANELS // 2, jnp.where(kind == 1, 0, kind // 2))
    half = jnp.where(kind == 0, lax.rem(k, 2), lax.rem(kind, 2))
    return kind, left, lax.rem(left + apart, PANELS), half


def on_or_above(width):
    i = lax.broadcasted_iota(jnp.int32, (width, width), 0)
    j = lax.broadcasted_iota(jnp.int32, (width, width), 1)
    return i, j


def exchange(
    N, R, rows, part, T, factor,
    w_hbm, x_hbm, m_ref, ag,
    w_ref, x_ref, xs, sbuf, own, dout, din, fo, up, fm,
    in_sems, a2a_s, a2a_r, sg_s, sg_r, dd_s, dd_r, up_s, fo_r, out_s, in_r, ag_s, near_r, far_r, rest_r, over_s,
):
    Z = N // 4
    CH = rows // part
    s = lax.axis_index("shift")
    r = lax.axis_index("row")
    core = lax.rem(s, 2)
    z = s // 4
    x = lax.rem(s // 2, 2)
    inputs = x_ref.shape[0]
    width = x_ref.shape[2]
    cut = width // 2
    piece = cut // PIECES
    U = T * PIECES
    slots = 2 * R
    G = 4 * R

    def member(x_, r_, c_):
        return (r_ * 2 + x_) * 2 + c_

    def place(z_, x_, c_):
        return (z_ * 2 + x_) * 2 + c_

    p = member(x, r, core)
    here = r * 2 + x
    partner = place(z, x, 1 - core)
    across = place(z, 1 - x, core)

    def row_at(i):
        return lax.rem(r + i + R, R)

    def remote(src, dst, ss, rr, to_s, to_r):
        return pltpu.make_async_remote_copy(
            src_ref=src, dst_ref=dst, send_sem=ss, recv_sem=rr,
            device_id={"shift": to_s, "row": to_r}, device_id_type=MESH,
        )

    def arrived(ref, sem):
        remote(ref, ref, a2a_s, sem, s, r).wait_recv()

    def left(ref, sem):
        remote(ref, ref, sem, rest_r, s, r).wait_send()

    load_x = pltpu.make_async_copy(x_hbm, x_ref, in_sems.at[0])
    load_w = pltpu.make_async_copy(w_hbm, w_ref, in_sems.at[1])
    load_x.start()
    load_w.start()
    barrier = pltpu.get_barrier_semaphore()
    for i in range(1, N):
        pl.semaphore_signal(barrier, inc=1, device_id={"shift": lax.rem(s + i, N), "row": r}, device_id_type=MESH)
    for i in range(1, R):
        for to in (s, across):
            pl.semaphore_signal(barrier, inc=1, device_id={"shift": to, "row": row_at(i)}, device_id_type=MESH)
    load_x.wait()
    load_w.wait()
    pl.semaphore_wait(barrier, N - 1 + 2 * (R - 1))


    def rows_of(owner, h):
        return pl.ds(pl.multiple_of(owner * rows + h * part, part), part)

    def send_rows(h, to):
        slot = lax.rem(to - s + N, N) - 1
        remote(x_ref.at[:, rows_of(to, h), :], xs.at[h, slot], a2a_s, a2a_r.at[h, jnp.where(slot < N // 2, 0, 1)], to, r).start()

    def send_chunk(h, c):
        for e in range(Z // 2):
            for to_z in (e, Z - 1 - e):
                for dx, dc in ((0, 0), (1, 0), (0, 1), (1, 1)):
                    to = place(to_z, lax.rem(x + dx, 2), lax.rem(core + dc, 2))
                    if dx or dc:
                        send_rows(h, to)
                    else:
                        @pl.when(to_z != z)
                        def _():
                            send_rows(h, to)
        return c

    lax.fori_loop(0, min(LEAD, CH), send_chunk, 0)


    def weigh(acc, blocks, source):
        parts = [b.astype(jnp.float32) for b in blocks]
        out = []
        for o in range(OUTS):
            base = (source * OUTS + o) * inputs
            total = parts[0] * w_ref[base]
            for c in range(1, inputs):
                total += parts[c] * w_ref[base + c]
            out.append(total if acc is None else acc[o] + total)
        return tuple(out)

    def panels_to(h, slot, sem, to_s, to_r):
        remote(sbuf.at[h, slot], sbuf.at[h, slot], sg_s, sem, to_s, to_r).start()

    def moments_of(h, c):
        acc = weigh(None, [x_ref[q, rows_of(s, h), :] for q in range(inputs)], s)
        arrived(xs.at[h, pl.ds(0, N // 2)], a2a_r.at[h, 0])

        def take(j, acc):
            return weigh(acc, [xs[h, j, q] for q in range(inputs)], lax.rem(s - 1 - j + N, N))

        acc = lax.fori_loop(0, N // 2, take, acc)
        arrived(xs.at[h, pl.ds(N // 2, N - 1 - N // 2)], a2a_r.at[h, 1])

        @pl.when(h + LEAD < CH)
        def _():
            send_chunk(h + LEAD, 0)

        acc = lax.fori_loop(N // 2, N - 1, take, acc)
        at = pl.ds(pl.multiple_of(h * part, part), part)
        for o in range(OUTS):
            value = acc[o].astype(jnp.bfloat16)
            sbuf[h, here, o] = value
            m_ref[o, at, :] = value
        for i in range(1, R):
            panels_to(h, here, sg_r, across, row_at(i))
        panels_to(h, here, sg_r, across, r)
        for i in range(1, R):
            panels_to(h, here, sg_r, s, row_at(i))

    def moments_direct(h, c):
        moments_of(h, c)
        return c

    lax.fori_loop(0, CH, moments_direct, 0)
    arrived(sbuf.at[:, pl.ds(0, slots - 1)], sg_r)


    depth = slots * rows

    def panel(k):
        return jnp.concatenate(
            [sbuf[:, :, k].reshape(depth, width), sbuf[:, :, PANELS + k].reshape(depth, width)], axis=1
        )

    def turned(k):
        return panel(k).T

    def product(a, b):
        v = jnp.dot(a, b, preferred_element_type=jnp.float32)
        return v[:width, :width] + v[width:, width:], v[:width, width:] - v[width:, :width]

    def halves(re, im):
        return [jnp.concatenate([re[h], im[h]], axis=1) for h in (slice(0, cut), slice(cut, width))]

    def packed(re, im):
        i, j = on_or_above(width)
        v = jnp.where(i <= j, re, im)
        return jnp.concatenate([v[:cut], v[cut:]], axis=1)

    def swap(t):
        return remote(dout.at[t], din.at[t], dd_s, dd_r.at[t], partner, r)

    def give(t, value):
        dout[t] = value.astype(jnp.bfloat16)
        swap(t).start()


    lower = z < Z // 2
    inner = jnp.where(lower, z + 1, z - 1)
    outer = jnp.where(lower, z - 1, z + 1)
    from_end = jnp.where(lower, z, Z - 1 - z)
    is_middle = from_end == Z // 2 - 1
    has_outer = from_end > 0
    inner_s = place(inner, x, core)
    outer_s = place(jnp.where(has_outer, outer, inner), x, core)

    def of(u):
        return u // PIECES, slice(u % PIECES * piece, u % PIECES * piece + piece)

    def climb(u):
        t, at = of(u)
        if u % PIECES == 0:
            arrived(din.at[t], dd_r.at[t])
        own[t, at] = (own[t, at] + din[t, at].astype(jnp.float32)) * factor

        @pl.when(has_outer)
        def _():
            arrived(fo.at[t, at], fo_r.at[u])
            own[t, at] = own[t, at] + fo[t, at].astype(jnp.float32)

        up[t, at] = own[t, at].astype(jnp.bfloat16)

        @pl.when(is_middle)
        def _():
            remote(up.at[t, at], fm.at[t, at], up_s, in_r.at[u], inner_s, r).start()

        @pl.when(jnp.logical_not(is_middle))
        def _():
            remote(up.at[t, at], fo.at[t, at], up_s, fo_r.at[u], inner_s, r).start()

    def forward(u, slot, sem, to_s, to_r):
        t, at = of(u)
        remote(ag.at[slot, t, at], ag.at[slot, t, at], ag_s, sem, to_s, to_r).start()

    def total(u):
        t, at = of(u)

        @pl.when(is_middle)
        def _():
            arrived(fm.at[t, at], in_r.at[u])
            ag[p, t, at] = (up[t, at].astype(jnp.float32) + fm[t, at].astype(jnp.float32)).astype(jnp.bfloat16)

        @pl.when(jnp.logical_not(is_middle))
        def _():
            arrived(ag.at[p, t, at], in_r.at[u])

        @pl.when(has_outer)
        def _():
            remote(ag.at[p, t, at], ag.at[p, t, at], out_s, in_r.at[u], outer_s, r).start()

    def close(u):
        return u >= U - CLOSE_PIECES

    over_z = [t for t in OVER_Z if t < T and not close(t * PIECES + PIECES - 1)] if Z > 2 and R > 1 else []

    def spread(u):
        forward(u, p, rest_r, partner, r)
        if close(u):
            for i in range(1, R):
                forward(u, p, far_r.at[u], across, row_at(i))
        ways = [(across, r)] + [(s, row_at(i)) for i in range(1, R)]
        for (to_s, to_r), (other_s, other_r) in zip(ways, reversed(ways)):
            forward(u, p, near_r.at[u], jnp.where(core == 0, to_s, other_s), jnp.where(core == 0, to_r, other_r))

    def finish(u):
        total(u)
        spread(u)

    def climb_and_finish(t):
        for u in range(t * PIECES, (t + 1) * PIECES):
            climb(u)
            if u >= SWAP_LAG:
                pl.when(is_middle)(functools.partial(finish, u - SWAP_LAG))

    other = member(x, r, 1 - core)
    if T == PANELS:
        low, high = halves(*product(turned(here), panel(here + PANELS // 2)))
        give(0, jnp.where(core == 0, high, low))
        own[0] = jnp.where(core == 0, low, high)
        a, b = turned(other), turned(p)
        give(1, packed(*product(a, panel(other))))
        own[1] = packed(*product(b, panel(p)))
        for d in range(1, PANELS // 2):
            low, high = halves(*product(a, panel(lax.rem(other + d, PANELS))))
            give(2 * d, low)
            give(2 * d + 1, high)
            climb_and_finish(2 * d - 2)
            climb_and_finish(2 * d - 1)
            own[2 * d], own[2 * d + 1] = halves(*product(b, panel(lax.rem(p + d, PANELS))))
        climb_and_finish(T - 2)
        climb_and_finish(T - 1)
    else:
        def unit(n):
            kind, k, q, half = unit_place(n)
            re, im = product(turned(k), panel(q))
            low, high = halves(re, im)
            return jnp.where(kind == 1, packed(re, im), jnp.where(half == 0, low, high))

        def theirs(t, c):
            give(t, unit(other * T + t))
            return c

        def mine(t, c):
            own[t] = unit(p * T + t)
            return c

        lax.fori_loop(0, T, theirs, 0)
        lax.fori_loop(0, T, mine, 0)
        for t in range(T):
            climb_and_finish(t)

    def relay(u):
        t, at = of(u)
        arrived(ag.at[pl.ds(0, R), t, at], near_r.at[u])
        forward(u, member(1 - x, r, core), rest_r, partner, r)
        for i in range(1, R):
            forward(u, member(x, row_at(-i), core), rest_r, partner, r)
        first = core == 0

        def to_diagonal():
            for i in range(1, R):
                slot = jnp.where(first, member(1 - x, r, core), member(x, row_at(-i), core))
                forward(u, slot, far_r.at[u], jnp.where(first, s, across), jnp.where(first, row_at(i), r))

        if t in over_z:
            pl.when(has_outer)(to_diagonal)
        elif not close(u):
            to_diagonal()

    def diagonal(u):
        t, at = of(u)
        arrived(ag.at[pl.ds(0, R - 1), t, at], far_r.at[u])
        for i in range(1, R):
            slot = member(1 - x, row_at(-i), core)
            if t in over_z:
                @pl.when(from_end == 1)
                def _():
                    remote(ag.at[slot, t, at], ag.at[slot, t, at], over_s, far_r.at[u], outer_s, r).start()
            forward(u, slot, rest_r, partner, r)

    for n in range(U + DIAGONAL_LAG):
        if n < U - SWAP_LAG:
            pl.when(jnp.logical_not(is_middle))(functools.partial(finish, n))
        elif n < U:
            finish(n)
        if 0 <= n - RELAY_LAG < U:
            relay(n - RELAY_LAG)
        if 0 <= n - DIAGONAL_LAG < U:
            diagonal(n - DIAGONAL_LAG)
    arrived(ag.at[pl.ds(0, slots)], rest_r)


    left(xs, a2a_s)
    left(sbuf.at[:, pl.ds(0, slots - 1)], sg_s)
    left(dout, dd_s)
    left(up, up_s)

    @pl.when(has_outer)
    def _():
        left(up, out_s)

    left(ag.at[pl.ds(0, G - 1), pl.ds(0, T - len(over_z))], ag_s)
    if over_z:
        left(ag.at[pl.ds(0, G - R), pl.ds(0, len(over_z))], ag_s)
        few = ag.at[pl.ds(0, R - 1), pl.ds(0, len(over_z))]

        @pl.when(has_outer)
        def _():
            left(few, ag_s)

        @pl.when(from_end == 1)
        def _():
            left(few, over_s)


def expand(T, m_in, ag_ref, m_out, re_out, im_out, re_buf, im_buf, sems, m_sem):
    width = re_buf.shape[1]
    half = PANELS // 2
    keep = pltpu.make_async_copy(m_in, m_out, m_sem)
    keep.start()

    def unit(n):
        return ag_ref[n // T, lax.rem(n, T)].astype(jnp.float32)

    def pair(k, d):
        v = jnp.concatenate([unit(PANELS * k + 2 * d), unit(PANELS * k + 2 * d + 1)], axis=0)
        return v[:, :width], v[:, width:]

    def writes(k, slot):
        at = pl.ds(pl.multiple_of(k * width, width), width)
        return (
            pltpu.make_async_copy(re_buf.at[k], re_out.at[at], sems.at[0, k]),
            pltpu.make_async_copy(im_buf.at[k], im_out.at[at], sems.at[1, k]),
        )

    def one(k, c):
        for d in range(PANELS):
            q = lax.rem(k + d, PANELS)
            at = pl.ds(pl.multiple_of(q * width, width), width)
            if d == 0:
                v = unit(PANELS * k + 1)
                v = jnp.concatenate([v[:, :width], v[:, width:]], axis=0)
                i, j = on_or_above(width)
                re = jnp.where(i <= j, v, v.T)
                im = jnp.where(i > j, v, jnp.where(i < j, -v.T, 0.0))
            elif d < half:
                re, im = pair(k, d)
            elif d == half:
                first = jnp.minimum(k, q)
                v = jnp.concatenate([unit(2 * PANELS * first), unit(2 * PANELS * first + PANELS)], axis=0)
                re, im = v[:, :width], v[:, width:]
                re, im = jnp.where(k < half, re, re.T), jnp.where(k < half, im, -im.T)
            else:
                re, im = pair(q, PANELS - d)
                re, im = re.T, -im.T
            re_buf[k, :, at] = re
            im_buf[k, :, at] = im
        for copy in writes(k, k):
            copy.start()
        return c

    lax.fori_loop(0, PANELS, one, 0)

    def finish(k, c):
        for copy in writes(k, k):
            copy.wait()
        return c

    lax.fori_loop(0, PANELS, finish, 0)
    keep.wait()


def local(N, R, solutions):
    shifts, parts, height, width = solutions.shape
    rows = height // N
    G = 4 * R
    T = UNITS // G
    assert T * G == UNITS
    cut = width // 2
    inputs = shifts * parts
    part = CHUNK_ROWS if rows % CHUNK_ROWS == 0 else rows
    chunks = rows // part
    factor = 1.0 / math.sqrt(height * R)
    w = jnp.asarray(coefficients(shifts * N, N))
    bf, dma = jnp.bfloat16, pltpu.SemaphoreType.DMA
    vmem = pl.BlockSpec(memory_space=pltpu.VMEM)
    hbm = pl.BlockSpec(memory_space=pltpu.HBM)
    unit = (T, cut, 2 * width)
    moments, parts_of_gram = pl.pallas_call(
        functools.partial(exchange, N, R, rows, part, T, factor),
        out_shape=(
            jax.ShapeDtypeStruct((OUTS, rows, width), bf),
            jax.ShapeDtypeStruct((G,) + unit, bf),
        ),
        in_specs=[hbm, hbm],
        out_specs=(vmem, vmem),
        scratch_shapes=[
            pltpu.SMEM(w.shape, jnp.float32),
            pltpu.VMEM((inputs, height, width), bf),
            pltpu.VMEM((chunks, N - 1, inputs, part, width), bf),
            pltpu.VMEM((chunks, 2 * R, OUTS, part, width), bf),
            pltpu.VMEM(unit, jnp.float32),
            pltpu.VMEM(unit, bf), pltpu.VMEM(unit, bf), pltpu.VMEM(unit, bf),
            pltpu.VMEM(unit, bf), pltpu.VMEM(unit, bf),
            dma((2,)),
            dma, dma((chunks, 2)), dma, dma,
            dma, dma((T,)), dma, dma((T * PIECES,)), dma, dma((T * PIECES,)),
            dma, dma((T * PIECES,)), dma((T * PIECES,)), dma, dma,
        ],
        compiler_params=pltpu.CompilerParams(
            collective_id=0, has_side_effects=True, vmem_limit_bytes=32 * 2**20
        ),
        cost_estimate=pl.CostEstimate(flops=10**9, bytes_accessed=2**23, transcendentals=0),
    )(
        pltpu.with_memory_space_constraint(w, pltpu.HBM),
        pltpu.with_memory_space_constraint(solutions.reshape(inputs, height, width), pltpu.HBM),
    )
    size = PANELS * width
    anywhere = pl.BlockSpec(memory_space=pl.ANY)
    moments, gram_real, gram_imag = pl.pallas_call(
        functools.partial(expand, T),
        out_shape=(
            jax.ShapeDtypeStruct((OUTS, rows, width), bf),
            jax.ShapeDtypeStruct((size, size), jnp.float32),
            jax.ShapeDtypeStruct((size, size), jnp.float32),
        ),
        in_specs=[vmem, vmem],
        out_specs=(anywhere, anywhere, anywhere),
        scratch_shapes=[
            pltpu.VMEM((PANELS, width, size), jnp.float32),
            pltpu.VMEM((PANELS, width, size), jnp.float32),
            dma((2, PANELS)),
            dma,
        ],
        compiler_params=pltpu.CompilerParams(vmem_limit_bytes=32 * 2**20),
        cost_estimate=pl.CostEstimate(flops=10**7, bytes_accessed=2**24, transcendentals=0),
    )(moments, parts_of_gram)
    return moments.reshape(2, PANELS, rows, width), gram_real, gram_imag


def solution(mesh):
    return jax.shard_map(
        functools.partial(local, mesh.shape["shift"], mesh.shape["row"]),
        mesh=mesh,
        in_specs=(P("shift", None, "row", None),),
        out_specs=(P(None, None, ("row", "shift"), None), P(), P()),
        check_vma=False,
    )
```
